32 devices in a mesh: obs: 8 (over z, y), chan: 4 (over x, core).
Axes of the slice: x: 2, y: 2, z: 4, core: 2. Of those that a mesh axis runs over, the one named last changes fastest.
Arguments:
- jacobian: bfloat16 [2048, 128, 137], P('obs', 'chan'), may hold values from -0.5 to 0.5
- departures: float32 [128, 2048], P('chan', 'obs'), may hold values from -6 to 6
- obs_weights: float32 [128, 2048], P('chan', 'obs'), may hold values from 0.25 to 4
- column_count: int32 [8], P('obs'), may hold values from 1 to 256, as said below
- grid_block: int32 [16], P('obs'), may hold values from 0 to 15, as said below
- sqrt_cov: float32 [137, 137], replicated, may hold values from -0.5 to 0.5
Outputs:
- increment: float32 [2048, 137], P('obs')
- residual: float32 [2048, 137], P('obs')
The draws below stay inside these ranges and needn't reach their ends.
Inputs may be any that keep to these rules, and one draw needn't show every extreme that they name: The first column_count of a device's 256 column slots are observed; some device has all 256 observed in every draw. `grid_block`: the owner of grid block g is index g // 2 of obs. The 2 blocks of one device match blocks of 2 different owners; in every draw some owner has a block matched by each device (every device matches one of that owner's blocks), and some device matches that owner's last block.
All inputs are finite; a program needn't handle non-finite values.
Results may differ from the reference program's by a relative error of at most 0.02.
Values may be sent and summed in bfloat16 or wider, within the bound.
A program may use at most 64 MiB of HBM per device.

```python
import math
import jax
import jax.numpy as jnp
from jax import lax

L = 137
BLOCK = 128
ITERS = 5
OBS_BLK = 2
GRID_BLK = 2
CHANNELS = 128
COLS = 2048
N_OBS = 8


def draw_column_count(key, part):
    span = OBS_BLK * BLOCK
    drawn = jax.random.randint(jax.random.fold_in(key, 11), (N_OBS,), 0, span + 1)
    counts = jnp.maximum(drawn * drawn // span, 1)
    fullest = jax.random.randint(jax.random.fold_in(key, 12), (), 0, N_OBS)
    counts = jnp.where(jnp.arange(N_OBS) == fullest, span, counts)
    return counts.astype(jnp.int32)


def draw_grid_block(key, part):
    common = jax.random.randint(jax.random.fold_in(key, 21), (), 0, N_OBS)
    scores = jax.random.randint(jax.random.fold_in(key, 22), (N_OBS, N_OBS), 0, 1048576)
    scores = scores * N_OBS + jnp.arange(N_OBS)[None, :]
    scores = jnp.where(jnp.arange(N_OBS)[None, :] == common, -1, scores)
    owners = jnp.argsort(scores, axis=1, stable=True)[:, :OBS_BLK]
    places = jax.random.randint(jax.random.fold_in(key, 23), (N_OBS, OBS_BLK), 0, GRID_BLK)
    chosen = jax.random.randint(jax.random.fold_in(key, 24), (), 0, N_OBS)
    rows = jnp.arange(N_OBS)[:, None]
    slots = jnp.arange(OBS_BLK)[None, :]
    places = jnp.where((rows == chosen) & (slots == 0), GRID_BLK - 1, places)
    return (owners * GRID_BLK + places).reshape(-1).astype(jnp.int32)


def steps_of(rng, extent, cuts, least, high):
    factor_of = 1.0
    for dim, blocks in cuts:
        draws = jax.random.uniform(jax.random.fold_in(jax.random.fold_in(rng, 6), dim), (blocks,), jnp.float32, least / len(cuts), high / len(cuts))
        factor_of = factor_of * jnp.repeat(jnp.exp(draws), extent[dim] // blocks).reshape((-1,) + (1,) * (len(extent) - 1 - dim))
    return factor_of


def scatter_about(stream_key, shape, scale, bound, cuts=(), held_as=jnp.bfloat16):
    result = scale * jax.random.normal(stream_key, shape, jnp.float32)
    if cuts:
        result = result * steps_of(stream_key, shape, cuts, -0.22, 0.18)
    return jnp.clip(result, -bound, bound).astype(held_as)


def setup_inputs(seed: int = 0) -> dict:
    arg_keys = jax.random.split(jax.random.key(seed), 7)
    jacobian = scatter_about(arg_keys[0], (COLS, CHANNELS, L), L ** -0.5, 0.5, ((0, 8), (1, 4)))
    departures = scatter_about(arg_keys[1], (CHANNELS, COLS), 1.0, 6.0, ((0, 4), (1, 8)), jnp.float32)
    obs_weights = jnp.clip(jnp.exp(math.log(4.0) - 2.7725887 * jax.random.uniform(arg_keys[2], (CHANNELS, COLS), jnp.float32) ** steps_of(arg_keys[2], (CHANNELS, COLS), ((0, 4), (1, 8)), -0.2, 0.2)), 0.25, 4.0)
    column_count = draw_column_count(jax.random.fold_in(arg_keys[6], 71), 0)
    grid_block = draw_grid_block(jax.random.fold_in(arg_keys[6], 71), 0)
    sqrt_cov = scatter_about(arg_keys[5], (L, L), L ** -0.5, 0.5, (), jnp.float32)
    return {"jacobian": jacobian, "departures": departures, "obs_weights": obs_weights, "column_count": column_count, "grid_block": grid_block, "sqrt_cov": sqrt_cov}


def source_block(operands):
    jac_part, weight_part, mask_part, depart_part = operands
    kernel = jac_part.astype(jnp.float32)
    scaled = (mask_part[:, None] * weight_part * depart_part).astype(jnp.bfloat16)
    scaled = lax.optimization_barrier(scaled).astype(jnp.float32)
    return jnp.einsum('cnl,cn->cl', kernel, scaled, precision=lax.Precision.HIGHEST)

def normal_block(operands):
    jac_part, weight_part, mask_part, field_part = operands
    kernel = jac_part.astype(jnp.float32)
    predicted = jnp.einsum('cnl,cl->cn', kernel, field_part.astype(jnp.float32), precision=lax.Precision.HIGHEST)
    scaled = (mask_part[:, None] * weight_part * predicted).astype(jnp.bfloat16)
    scaled = lax.optimization_barrier(scaled).astype(jnp.float32)
    return jnp.einsum('cnl,cn->cl', kernel, scaled, precision=lax.Precision.HIGHEST)

def reference(jacobian, departures, obs_weights, column_count, grid_block, sqrt_cov):
    columns_all = jacobian.shape[0]
    per_device = OBS_BLK * BLOCK
    position = jnp.arange(columns_all, dtype=jnp.int32)
    observed = (position % per_device < column_count[position // per_device]).astype(jnp.float32)
    block_total = columns_all // BLOCK
    jac_blocks = jacobian.reshape(block_total, BLOCK, CHANNELS, L)
    weight_blocks = obs_weights.T.reshape(block_total, BLOCK, CHANNELS)
    depart_blocks = departures.T.reshape(block_total, BLOCK, CHANNELS)
    mask_blocks = observed.reshape(block_total, BLOCK)
    grid_total = GRID_BLK * N_OBS

    def collect(terms):
        summed = jnp.zeros((grid_total, BLOCK, L), jnp.float32).at[grid_block].add(terms)
        return summed.reshape(grid_total * BLOCK, L)

    def spread(field):
        return jnp.dot(field, sqrt_cov, precision=lax.Precision.HIGHEST)

    def spread_back(field):
        return jnp.dot(field, sqrt_cov.T, precision=lax.Precision.HIGHEST)

    def normal(direction):
        rounded = lax.optimization_barrier(spread(direction).astype(jnp.bfloat16))
        fields = rounded.reshape(grid_total, BLOCK, L)[grid_block]
        terms = lax.map(normal_block, (jac_blocks, weight_blocks, mask_blocks, fields))
        return direction + spread_back(collect(terms))
    source_terms = lax.map(source_block, (jac_blocks, weight_blocks, mask_blocks, depart_blocks))
    residual = spread_back(collect(source_terms))
    control = jnp.zeros_like(residual)
    direction = residual
    norm_now = jnp.sum(residual * residual)
    for iteration in range(ITERS):
        image = normal(direction)
        step_length = norm_now / jnp.sum(direction * image)
        control = control + step_length * direction
        residual = residual - step_length * image
        norm_next = jnp.sum(residual * residual)
        direction = residual + norm_next / norm_now * direction
        norm_now = norm_next
    return (spread(control), residual)
```

```python
import functools
import jax
import jax.numpy as jnp
from jax import lax
from jax.experimental import pallas as pl
from jax.experimental.pallas import tpu as pltpu
from jax.sharding import PartitionSpec as P

BLOCK = 128
ITERS = 5
GRID_BLK = 2
HIGHEST = lax.Precision.HIGHEST
MESH = pl.DeviceIdType.MESH


def block_terms(jac_part, weight_part, mask_part, predicted):
    scaled = (mask_part[:, None] * weight_part * predicted).astype(jnp.bfloat16)
    return lax.dot_general(
        jac_part, scaled, (((1,), (1,)), ((0,), (0,))), preferred_element_type=jnp.float32
    )


def forward_terms(jac_part, weight_part, mask_part, field_part):
    predicted = lax.dot_general(
        jac_part, field_part, (((2,), (1,)), ((0,), (0,))), preferred_element_type=jnp.float32
    )
    return block_terms(jac_part, weight_part, mask_part, predicted)


def exchange_per_step(jacobian, departures, obs_weights, column_count, grid_block, sqrt_cov):
    obs_count = lax.axis_size("obs")
    myself = lax.axis_index("obs")
    capacity, group_channels, layers = jacobian.shape
    block_count = capacity // BLOCK
    weight_cols = obs_weights.T
    depart_cols = departures.T
    observed = (jnp.arange(capacity, dtype=jnp.int32) < column_count[0]).astype(jnp.float32)
    every_id = lax.all_gather(grid_block, "obs", axis=0, tiled=True).reshape(obs_count, block_count)
    targets = jnp.arange(obs_count, dtype=jnp.int32)
    send_pick = (grid_block[None, :] // GRID_BLK == targets[:, None]).astype(jnp.float32)
    owned_here = every_id // GRID_BLK == myself
    places = every_id % GRID_BLK
    grid_index = jnp.arange(GRID_BLK, dtype=jnp.int32)
    take_pick = jnp.sum(
        ((places[None] == grid_index[:, None, None]) & owned_here[None]).astype(jnp.float32), axis=2
    )
    share_cols = BLOCK

    def local_terms(kernel_fn, inputs):
        return kernel_fn(jacobian, weight_cols, observed, inputs)

    def to_owners(terms):
        blocked = terms.reshape(block_count, BLOCK, layers)
        blocked = lax.psum(blocked, "chan")
        outgoing = jnp.dot(
            send_pick, blocked.reshape(block_count, -1), precision=lax.Precision.HIGHEST
        )
        incoming = lax.all_to_all(
            outgoing.reshape(obs_count, share_cols, layers),
            "obs",
            split_axis=0,
            concat_axis=0,
            tiled=True,
        )
        summed = jnp.dot(
            take_pick, incoming.reshape(obs_count, -1), precision=lax.Precision.HIGHEST
        )
        return summed.reshape(GRID_BLK, share_cols, layers)

    def spread(field):
        return jnp.dot(
            field.reshape(-1, layers), sqrt_cov, precision=lax.Precision.HIGHEST
        ).reshape(field.shape)

    def spread_back(field):
        flat = lax.dot_general(
            field.reshape(-1, layers),
            sqrt_cov,
            (((1,), (1,)), ((), ())),
            precision=lax.Precision.HIGHEST,
        )
        return flat.reshape(field.shape)

    def squared(values):
        partial_sum = jnp.sum(values * values)
        return lax.psum(partial_sum, "obs")

    residual = spread_back(to_owners(local_terms(block_terms, depart_cols)))
    control = jnp.zeros_like(residual)
    direction = residual
    norm_now = squared(residual)
    for iteration in range(ITERS):
        rounded = spread(direction).astype(jnp.bfloat16).reshape(GRID_BLK, -1)
        to_outgoing = jnp.dot(
            take_pick.T.astype(jnp.bfloat16), rounded, preferred_element_type=jnp.float32
        ).astype(jnp.bfloat16)
        to_incoming = lax.all_to_all(
            to_outgoing.reshape(obs_count, share_cols, layers),
            "obs",
            split_axis=0,
            concat_axis=0,
            tiled=True,
        )
        picked = jnp.dot(
            send_pick.T.astype(jnp.bfloat16),
            to_incoming.reshape(obs_count, -1),
            preferred_element_type=jnp.float32,
        )
        picked = picked.astype(jnp.bfloat16).reshape(block_count, share_cols, layers)
        fetched = picked.reshape(capacity, layers)
        image = direction + spread_back(to_owners(local_terms(forward_terms, fetched)))
        curvature_partial_sum = jnp.sum(direction * image)
        step_length = norm_now / lax.psum(curvature_partial_sum, "obs")
        control = control + step_length * direction
        residual = residual - step_length * image
        norm_next = squared(residual)
        direction = residual + norm_next / norm_now * direction
        norm_now = norm_next
    increment = spread(control)
    return (increment.reshape(-1, layers), residual.reshape(-1, layers))


LANES = 128
SUB = 8
PIECE = 3
STEPS = ITERS + 1
NT = (((1,), (1,)), ((), ()))
TN = (((0,), (0,)), ((), ()))


def exact_dot(a, b, dims):
    return lax.dot_general(a, b, dims, precision=HIGHEST, preferred_element_type=jnp.float32)


def one_hot_dot(a, b, dims=NT):
    return lax.dot_general(a, b, dims, preferred_element_type=jnp.float32)


def cg_kernel(
    obs_count, chan_count, jac_ref, obs_weight_ref, depart_ref, count_ref, block_ref, cov_ref,
    increment_ref, residual_ref,
    jac_vmem, put_ref, got_ref, kernel_ref, weight_ref, order_ref, back_order_ref, gram_ref, cov_pad_ref,
    relation_ref, id_ref, terms_ref, parts_ref, back_ref,
    load_sem, jac_send, jac_recv, id_send, id_recv, term_send, term_recv, sum_send, sum_recv, back_send, back_recv
):
    layers, channels, columns = jac_ref.shape
    padded = jac_vmem.shape[0]
    chunk_count = padded // SUB
    piece_count = chunk_count // PIECE
    half_obs = obs_count // 2
    group = half_obs * chan_count
    rows = kernel_ref.shape[0]
    lows = chan_count // 2
    block_count = columns // BLOCK
    mine = block_count * SUB

    obs, chan = lax.axis_index("obs"), lax.axis_index("chan")
    top = obs // half_obs
    me = (obs % half_obs) * chan_count + chan
    slot = (chan % lows) * (2 * half_obs) + (chan // lows) * half_obs + obs % half_obs

    def coords(member):
        return (top * half_obs + member // chan_count, member % chan_count)

    def other(k):
        member, place = 0, 1
        while place < group:
            member = member + (me // place + k // place) % 2 * place
            place *= 2
        return member

    partner = ((obs + half_obs) % obs_count, chan)
    barrier = pltpu.get_barrier_semaphore()

    def greet(k, carry):
        pl.semaphore_signal(barrier, inc=1, device_id=coords(other(k)), device_id_type=MESH)
        return carry

    lax.fori_loop(1, group, greet, 0)
    pl.semaphore_signal(barrier, inc=1, device_id=partner, device_id_type=MESH)

    order_of_chunks = [chunk_count - 1] + list(range(chunk_count - 1))
    pieces = [order_of_chunks[PIECE * p : PIECE * (p + 1)] for p in range(piece_count)]
    loads, sem_index = [], 0
    for piece in pieces:
        runs = [piece] if piece[0] != chunk_count - 1 else [piece[:1], piece[1:]]
        copies = []
        for run in runs:
            first, last = run[0] * SUB, min((run[-1] + 1) * SUB, layers)
            part = pl.ds(first, last - first)
            copies.append(pltpu.make_async_copy(jac_ref.at[part], jac_vmem.at[part], load_sem.at[sem_index]))
            sem_index += 1
        loads.append(copies)
    for copies in loads:
        for copy in copies:
            copy.start()

    place = lax.broadcasted_iota(jnp.int32, (channels, columns), 1)
    weight = jnp.where(place < count_ref[0], obs_weight_ref[...], 0.0)
    weight_high = weight.astype(jnp.bfloat16)
    jac_vmem[layers] = weight_high
    jac_vmem[layers + 1] = (weight - weight_high.astype(jnp.float32)).astype(jnp.bfloat16)
    jac_vmem[layers + 2] = (weight * depart_ref[...]).astype(jnp.bfloat16)
    ids = jnp.zeros((channels, columns), jnp.float32)
    for k in range(block_count):
        ids = jnp.where(place // BLOCK == k, block_ref[k].astype(jnp.float32), ids)
    jac_vmem[layers + 3] = ids.astype(jnp.bfloat16)
    for extra in range(layers + 4, padded):
        jac_vmem[extra] = jnp.zeros((channels, columns), jnp.bfloat16)

    def one_hot(shape, wanted):
        row = lax.broadcasted_iota(jnp.int32, shape, 0)
        column = lax.broadcasted_iota(jnp.int32, shape, 1)
        return jnp.where(column == wanted(row), 1.0, 0.0).astype(jnp.bfloat16)

    order_ref[...] = one_hot(
        (columns, columns), lambda r: r % mine // SUB * BLOCK + r // mine * SUB + r % SUB
    )
    width = SUB * channels
    back_order_ref[...] = one_hot((width, width), lambda r: r % SUB * channels + r // SUB)

    def stage(p):
        for copy in loads[p]:
            copy.wait()
        for i, chunk in enumerate(pieces[p]):
            block = jac_vmem[chunk * SUB : (chunk + 1) * SUB].reshape(width, columns)
            turned = one_hot_dot(order_ref[...], block).astype(jnp.bfloat16)
            put_ref[p, :, i] = turned.reshape(group, mine, width)

    def send(p):
        def one(k, carry):
            member = other(k)
            pltpu.make_async_remote_copy(
                src_ref=put_ref.at[p, member],
                dst_ref=got_ref.at[p, slot],
                send_sem=jac_send.at[p],
                recv_sem=jac_recv.at[p],
                device_id=coords(member),
                device_id_type=MESH,
            ).start()
            return carry

        lax.fori_loop(1, group, one, 0)
        got_ref[p, slot] = put_ref[p, me]

    stage(0)
    pl.semaphore_wait(barrier, group)
    for p in range(piece_count):
        if p:
            stage(p)
        send(p)

    cov = cov_ref[...]
    gram_ref[...] = jnp.zeros((padded, padded), jnp.float32)
    cov_pad_ref[...] = jnp.zeros((padded, padded), jnp.float32)
    gram_ref[0:layers, 0:layers] = exact_dot(cov, cov, TN)
    cov_pad_ref[0:layers, 0:layers] = cov

    def take(p):
        others = got_ref.at[p, pl.ds(0, group - 1)]
        pltpu.make_async_copy(others, others, jac_recv.at[p]).wait()
        for i, chunk in enumerate(pieces[p]):
            block = got_ref[p, :, i].reshape(group * mine, width)
            turned = one_hot_dot(back_order_ref[...], block)
            for low in range(lows):
                part = turned[:, low * LANES : (low + 1) * LANES].reshape(channels, SUB, LANES)
                kernel_ref[low * channels : (low + 1) * channels, chunk * SUB : (chunk + 1) * SUB, :] = part

    take(0)
    lane_row = lax.broadcasted_iota(jnp.int32, (SUB, LANES), 1)
    weight_ref[...] = kernel_ref[:, layers, :] + kernel_ref[:, layers + 1, :]
    id_ref[0] = jnp.broadcast_to(kernel_ref[0, layers + 3 : layers + 4, :], (SUB, LANES))
    id_copy = pltpu.make_async_remote_copy(
        src_ref=id_ref.at[0], dst_ref=id_ref.at[1], send_sem=id_send, recv_sem=id_recv,
        device_id=partner, device_id_type=MESH,
    )
    id_copy.start()
    for p in range(1, piece_count - 1):
        take(p)

    id_copy.wait()
    grid_row = lax.broadcasted_iota(jnp.int32, (LANES, LANES), 0)
    grid_lane = lax.broadcasted_iota(jnp.int32, (LANES, LANES), 1)

    def pick_of(which):
        wanted = id_ref[which, 0:1, :].astype(jnp.int32) * SUB + grid_lane % SUB
        return jnp.where(grid_row == wanted, 1.0, 0.0).astype(jnp.bfloat16)

    own_pick = pick_of(0)
    both_picks = jnp.concatenate([own_pick, pick_of(1)], axis=1)
    matched = one_hot_dot(own_pick, both_picks, TN).astype(jnp.bfloat16)
    relation = jnp.concatenate([both_picks, matched], axis=0).astype(jnp.float32)
    relation_lane = lax.broadcasted_iota(jnp.int32, relation.shape, 1) % LANES
    for which in range(2):
        kept = relation_lane // (LANES // 2) == which
        relation_ref[which] = jnp.where(kept, relation, 0.0).astype(jnp.bfloat16)

    take(piece_count - 1)

    half_rows = padded // 2
    lane = lax.broadcasted_iota(jnp.int32, (half_rows, LANES), 1)
    zero = jnp.zeros((padded, LANES), jnp.float32)

    def terms_copy(step):
        return pltpu.make_async_remote_copy(
            src_ref=terms_ref.at[step, 0], dst_ref=terms_ref.at[step, 1],
            send_sem=term_send.at[step], recv_sem=term_recv.at[step],
            device_id=partner, device_id_type=MESH,
        )

    def put_terms(step, terms):
        summed = terms + pltpu.roll(terms, LANES // 2, 1)
        packed = jnp.where(lane < LANES // 2, summed[:half_rows], summed[half_rows:])
        terms_ref[step, 0] = packed
        terms_copy(step).start()

    def collected(step):
        terms_copy(step).wait()
        both = jnp.concatenate([terms_ref[step, 0], terms_ref[step, 1]], axis=1)
        high = both.astype(jnp.bfloat16)
        low = (both - high.astype(jnp.float32)).astype(jnp.bfloat16)
        parts = jnp.concatenate([high.astype(jnp.float32), low.astype(jnp.float32)], axis=0).astype(jnp.bfloat16)
        sums = [one_hot_dot(parts, relation_ref[which]) for which in range(2)]
        return jnp.concatenate([value[:half_rows] + value[half_rows:] for value in sums], axis=0)

    def source_step(n, acc):
        kernel = kernel_ref[n]
        return acc + kernel * kernel[layers + 2 : layers + 3]

    def put_normal(step, spread):
        def normal_step(n, acc):
            kernel = kernel_ref[n]
            predicted = jnp.sum(kernel * spread, axis=0, keepdims=True)
            return acc + kernel * (predicted * weight_ref[pl.ds(n, 1), :])

        put_terms(step, lax.fori_loop(0, rows, normal_step, zero, unroll=4))

    def gram_dot(field):
        return exact_dot(gram_ref[...], field, (((1,), (0,)), ((), ())))

    put_terms(0, lax.fori_loop(0, rows, source_step, zero, unroll=4))
    residual_both = collected(0)
    spread_both = gram_dot(residual_both)
    residual, spread = residual_both[:, :LANES], spread_both[:, :LANES]
    put_normal(1, spread_both[:, LANES:])
    applied_both = residual_both + collected(1)
    control = direction = image = spread_image = image_applied = None
    norm_last = step_last = None
    for step in range(ITERS):
        applied = applied_both[:, :LANES]
        norm_part = jnp.sum(residual * spread, axis=0, keepdims=True)
        curve_part = jnp.sum(applied * spread, axis=0, keepdims=True)
        parts_ref[step, me, 0:1] = norm_part
        parts_ref[step, me, 1:2] = curve_part

        def send_sum(k, carry, step=step):
            pltpu.make_async_remote_copy(
                src_ref=parts_ref.at[step, me],
                dst_ref=parts_ref.at[step, me],
                send_sem=sum_send.at[step],
                recv_sem=sum_recv.at[step],
                device_id=coords(other(k)),
                device_id_type=MESH,
            ).start()
            return carry

        lax.fori_loop(1, group, send_sum, 0)
        last = step == ITERS - 1
        if not last:
            next_spread = gram_dot(applied_both)
            put_normal(step + 2, next_spread[:, LANES:])
        others = parts_ref.at[step, pl.ds(0, group - 1)]
        pltpu.make_async_copy(others, others, sum_recv.at[step]).wait()
        pltpu.make_async_copy(others, others, sum_send.at[step]).wait()
        total = jnp.sum(parts_ref[step], axis=0)
        total = jnp.sum(total, axis=1, keepdims=True)
        norm_now, curve = total[0:1], total[1:2]
        if step == 0:
            length = norm_now / curve
            direction, image = residual, applied
            control = length * direction
        else:
            ratio = norm_now / norm_last
            length = norm_now / (curve - ratio * norm_now / step_last)
            direction = residual + ratio * direction
            image = applied + ratio * image
            control = control + length * direction
        residual = residual - length * image
        if not last:
            if step == 0:
                spread_image = next_spread[:, :LANES]
                image_applied = applied_both + collected(step + 2)
            else:
                spread_image = next_spread[:, :LANES] + ratio * spread_image
                image_applied = applied_both + collected(step + 2) + ratio * image_applied
            spread = spread - length * spread_image
            applied_both = applied_both - length * image_applied
        norm_last, step_last = norm_now, length

    outs = (exact_dot(control, gram_ref[...], TN), exact_dot(residual, cov_pad_ref[...], (((0,), (1,)), ((), ()))))
    for which, out in enumerate(outs):
        value = out.astype(jnp.bfloat16).reshape(obs_count, GRID_BLK, SUB, padded)
        back_ref[0, 0:obs_count, which] = value

    def back_source(member):
        return back_ref.at[0, top * half_obs + member // chan_count]

    def send_back(k, carry):
        member = other(k)
        pltpu.make_async_remote_copy(
            src_ref=back_source(member),
            dst_ref=back_ref.at[1, me],
            send_sem=back_send,
            recv_sem=back_recv,
            device_id=coords(member),
            device_id_type=MESH,
        ).start()
        return carry

    lax.fori_loop(1, group, send_back, 0)
    back_ref[1, me] = back_ref[0, obs]
    for p in range(piece_count):
        others = put_ref.at[p, pl.ds(0, group - 1)]
        pltpu.make_async_copy(others, others, jac_send.at[p]).wait()
    others = back_ref.at[1, pl.ds(0, group - 1)]
    pltpu.make_async_copy(others, others, back_recv).wait()
    pltpu.make_async_copy(others, others, back_send).wait()
    straight = one_hot((padded, padded), lambda r: r)
    for which, out_ref in enumerate((increment_ref, residual_ref)):
        for block in range(GRID_BLK):
            value = back_ref[1, :, which, block].reshape(group * SUB, padded)
            turned = one_hot_dot(straight, value)
            out_ref[:, block * BLOCK : (block + 1) * BLOCK] = turned[:layers]


def half_slice_columns(jacobian, departures, obs_weights, column_count, grid_block, sqrt_cov):
    obs_count, chan_count = lax.axis_size("obs"), lax.axis_size("chan")
    group = obs_count // 2 * chan_count
    capacity, channels, layers = jacobian.shape
    mine = capacity // BLOCK * SUB
    padded = LANES + 2 * SUB
    chunk_count = padded // SUB
    piece_count = chunk_count // PIECE
    rows = channels * chan_count // 2
    width = SUB * channels

    out = jax.ShapeDtypeStruct((layers, GRID_BLK * BLOCK), jnp.float32)
    vmem = pl.BlockSpec(memory_space=pltpu.VMEM)
    smem = pl.BlockSpec(memory_space=pltpu.SMEM)
    dma = pltpu.SemaphoreType.DMA
    bf16, f32 = jnp.bfloat16, jnp.float32
    increment, residual = pl.pallas_call(
        functools.partial(cg_kernel, obs_count, chan_count),
        out_shape=(out, out),
        in_specs=[pl.BlockSpec(memory_space=pl.ANY), vmem, vmem, smem, smem, vmem],
        out_specs=(vmem, vmem),
        scratch_shapes=[
            pltpu.VMEM((padded, channels, capacity), bf16),
            pltpu.VMEM((piece_count, group, PIECE, mine, width), bf16),
            pltpu.VMEM((piece_count, group, PIECE, mine, width), bf16),
            pltpu.VMEM((rows, padded, LANES), f32),
            pltpu.VMEM((rows, LANES), f32),
            pltpu.VMEM((capacity, capacity), bf16),
            pltpu.VMEM((width, width), bf16),
            pltpu.VMEM((padded, padded), f32),
            pltpu.VMEM((padded, padded), f32),
            pltpu.VMEM((2, 2 * LANES, 2 * LANES), bf16),
            pltpu.VMEM((2, SUB, LANES), f32),
            pltpu.VMEM((STEPS, 2, padded // 2, LANES), f32),
            pltpu.VMEM((ITERS, group, 2, LANES), f32),
            pltpu.VMEM((2, group, 2, GRID_BLK, SUB, padded), bf16),
            dma((piece_count + 1,)),
            dma((piece_count,)), dma((piece_count,)),
            dma, dma,
            dma((STEPS,)), dma((STEPS,)),
            dma((ITERS,)), dma((ITERS,)),
            dma, dma,
        ],
        compiler_params=pltpu.CompilerParams(
            collective_id=0, has_side_effects=True, vmem_limit_bytes=50 * 1024 * 1024
        ),
    )(jacobian.transpose(2, 1, 0), obs_weights, departures, column_count, grid_block, sqrt_cov)
    return increment.T, residual.T


def solution(mesh):
    obs_count, chan_count = mesh.shape["obs"], mesh.shape["chan"]
    group = obs_count // 2 * chan_count

    def plan(jacobian, departures, obs_weights, column_count, grid_block, sqrt_cov):
        capacity, channels, layers = jacobian.shape
        mine = capacity // BLOCK * SUB
        fits = (
            obs_count % 2 == 0
            and chan_count % 2 == 0
            and group * SUB == BLOCK
            and obs_count * mine == LANES
            and obs_count * GRID_BLK * SUB == LANES
            and chan_count == 4
            and channels == 32
            and LANES + SUB < layers + 4 <= LANES + 2 * SUB
        )
        chosen = half_slice_columns if fits else exchange_per_step
        return chosen(jacobian, departures, obs_weights, column_count, grid_block, sqrt_cov)

    in_specs = (P("obs", "chan", None), P("chan", "obs"), P("chan", "obs"), P("obs"), P("obs"), P())
    out_specs = (P("obs", None), P("obs", None))
    return jax.shard_map(plan, mesh=mesh, in_specs=in_specs, out_specs=out_specs, check_vma=False)
```

```python
import contextlib
import functools
import jax
import jax.numpy as jnp
from jax import lax
from jax.experimental import pallas as pl
from jax.experimental.pallas import tpu as pltpu
from jax.sharding import PartitionSpec as P

BLOCK = 128
ITERS = 5
GRID_BLK = 2
HIGHEST = lax.Precision.HIGHEST
MESH = pl.DeviceIdType.MESH


def block_terms(jac_part, weight_part, mask_part, predicted):
    scaled = (mask_part[:, None] * weight_part * predicted).astype(jnp.bfloat16)
    return lax.dot_general(
        jac_part, scaled, (((1,), (1,)), ((0,), (0,))), preferred_element_type=jnp.float32
    )


def forward_terms(jac_part, weight_part, mask_part, field_part):
    predicted = lax.dot_general(
        jac_part, field_part, (((2,), (1,)), ((0,), (0,))), preferred_element_type=jnp.float32
    )
    return block_terms(jac_part, weight_part, mask_part, predicted)


def exchange_per_step(jacobian, departures, obs_weights, column_count, grid_block, sqrt_cov):
    obs_count = lax.axis_size("obs")
    myself = lax.axis_index("obs")
    capacity, group_channels, layers = jacobian.shape
    block_count = capacity // BLOCK
    weight_cols = obs_weights.T
    depart_cols = departures.T
    observed = (jnp.arange(capacity, dtype=jnp.int32) < column_count[0]).astype(jnp.float32)
    every_id = lax.all_gather(grid_block, "obs", axis=0, tiled=True).reshape(obs_count, block_count)
    targets = jnp.arange(obs_count, dtype=jnp.int32)
    send_pick = (grid_block[None, :] // GRID_BLK == targets[:, None]).astype(jnp.float32)
    owned_here = every_id // GRID_BLK == myself
    places = every_id % GRID_BLK
    grid_index = jnp.arange(GRID_BLK, dtype=jnp.int32)
    take_pick = jnp.sum(
        ((places[None] == grid_index[:, None, None]) & owned_here[None]).astype(jnp.float32), axis=2
    )
    share_cols = BLOCK

    def local_terms(kernel_fn, inputs):
        return kernel_fn(jacobian, weight_cols, observed, inputs)

    def to_owners(terms):
        blocked = terms.reshape(block_count, BLOCK, layers)
        blocked = lax.psum(blocked, "chan")
        outgoing = jnp.dot(
            send_pick, blocked.reshape(block_count, -1), precision=lax.Precision.HIGHEST
        )
        incoming = lax.all_to_all(
            outgoing.reshape(obs_count, share_cols, layers),
            "obs",
            split_axis=0,
            concat_axis=0,
            tiled=True,
        )
        summed = jnp.dot(
            take_pick, incoming.reshape(obs_count, -1), precision=lax.Precision.HIGHEST
        )
        return summed.reshape(GRID_BLK, share_cols, layers)

    def spread(field):
        return jnp.dot(
            field.reshape(-1, layers), sqrt_cov, precision=lax.Precision.HIGHEST
        ).reshape(field.shape)

    def spread_back(field):
        flat = lax.dot_general(
            field.reshape(-1, layers),
            sqrt_cov,
            (((1,), (1,)), ((), ())),
            precision=lax.Precision.HIGHEST,
        )
        return flat.reshape(field.shape)

    def squared(values):
        partial_sum = jnp.sum(values * values)
        return lax.psum(partial_sum, "obs")

    residual = spread_back(to_owners(local_terms(block_terms, depart_cols)))
    control = jnp.zeros_like(residual)
    direction = residual
    norm_now = squared(residual)
    for iteration in range(ITERS):
        rounded = spread(direction).astype(jnp.bfloat16).reshape(GRID_BLK, -1)
        to_outgoing = jnp.dot(
            take_pick.T.astype(jnp.bfloat16), rounded, preferred_element_type=jnp.float32
        ).astype(jnp.bfloat16)
        to_incoming = lax.all_to_all(
            to_outgoing.reshape(obs_count, share_cols, layers),
            "obs",
            split_axis=0,
            concat_axis=0,
            tiled=True,
        )
        picked = jnp.dot(
            send_pick.T.astype(jnp.bfloat16),
            to_incoming.reshape(obs_count, -1),
            preferred_element_type=jnp.float32,
        )
        picked = picked.astype(jnp.bfloat16).reshape(block_count, share_cols, layers)
        fetched = picked.reshape(capacity, layers)
        image = direction + spread_back(to_owners(local_terms(forward_terms, fetched)))
        curvature_partial_sum = jnp.sum(direction * image)
        step_length = norm_now / lax.psum(curvature_partial_sum, "obs")
        control = control + step_length * direction
        residual = residual - step_length * image
        norm_next = squared(residual)
        direction = residual + norm_next / norm_now * direction
        norm_now = norm_next
    increment = spread(control)
    return (increment.reshape(-1, layers), residual.reshape(-1, layers))


LANES = 128
SUB = 8
PIECE = 3
VMEM_BYTES = 67043328 - 1024 * 1024
STEPS = ITERS + 1
scope = lambda name: contextlib.nullcontext()
NT = (((1,), (1,)), ((), ()))
TN = (((0,), (0,)), ((), ()))


def exact_dot(a, b, dims):
    return lax.dot_general(a, b, dims, precision=HIGHEST, preferred_element_type=jnp.float32)


def one_hot_dot(a, b, dims=NT):
    return lax.dot_general(a, b, dims, preferred_element_type=jnp.float32)


def cg_kernel(
    obs_count, chan_count, jac_ref, *rest
):
    smalls, (increment_ref, residual_ref), rest = rest[:5], rest[5:7], rest[7:]
    run_cg(obs_count, chan_count, jac_ref, smalls, rest[:5], increment_ref, residual_ref, *rest[5:])


def run_cg(
    obs_count, chan_count, jac_ref, small_hbm, small_refs, increment_ref, residual_ref,
    jac_vmem, source_ref, mixed_ref, put_ref, got_ref, kernel_ref, weight_ref, order_ref, back_order_ref,
    gram_ref, out_maps_ref, spread_ref, predicted_ref, relation_ref, id_ref, terms_ref, parts_ref, finals_ref, back_ref,
    small_sem, load_sem, jac_send, jac_recv, id_send, id_recv, term_send, term_recv, sum_send, sum_recv,
    final_send, final_recv, back_send, back_recv
):
    obs_weight_ref, depart_ref, count_ref, block_ref, cov_ref = small_refs
    small_loads = [
        pltpu.make_async_copy(source, target, small_sem.at[i])
        for i, (source, target) in enumerate(zip(small_hbm, small_refs))
    ]
    for copy in small_loads:
        copy.start()
    layers, channels, columns = jac_ref.shape
    padded = jac_vmem.shape[0]
    chunk_count = padded // SUB
    piece_count = chunk_count // PIECE
    half_obs = obs_count // 2
    group = half_obs * chan_count
    rows = kernel_ref.shape[0]
    lows = chan_count // 2
    block_count = columns // BLOCK
    mine = block_count * SUB

    obs, chan = lax.axis_index("obs"), lax.axis_index("chan")
    top = obs // half_obs
    me = (obs % half_obs) * chan_count + chan
    slot = (chan % lows) * (2 * half_obs) + (chan // lows) * half_obs + obs % half_obs

    def coords(member):
        return (top * half_obs + member // chan_count, member % chan_count)

    def other(k):
        member, place = 0, 1
        while place < group:
            member = member + (me // place + k // place) % 2 * place
            place *= 2
        return member

    device_count = obs_count * chan_count
    rank = obs * chan_count + chan

    def any_other(k):
        member, place = 0, 1
        while place < device_count:
            member = member + (rank // place + k // place) % 2 * place
            place *= 2
        return (member // chan_count, member % chan_count)

    partner = ((obs + half_obs) % obs_count, chan)
    barrier = pltpu.get_barrier_semaphore()

    def greet(k, carry):
        pl.semaphore_signal(barrier, inc=1, device_id=coords(other(k)), device_id_type=MESH)
        return carry

    lax.fori_loop(1, group, greet, 0)
    pl.semaphore_signal(barrier, inc=1, device_id=partner, device_id_type=MESH)

    order_of_chunks = [chunk_count - 1] + list(range(chunk_count - 1))
    pieces = [order_of_chunks[PIECE * p : PIECE * (p + 1)] for p in range(piece_count)]
    loads, sem_index = [], 0
    for piece in pieces:
        runs = [piece] if piece[0] != chunk_count - 1 else [piece[:1], piece[1:]]
        copies = []
        for run in runs:
            first, last = run[0] * SUB, min((run[-1] + 1) * SUB, layers)
            part = pl.ds(first, last - first)
            copies.append(pltpu.make_async_copy(jac_ref.at[part], jac_vmem.at[part], load_sem.at[sem_index]))
            sem_index += 1
        loads.append(copies)
    for copies in loads:
        for copy in copies:
            copy.start()

    for copy in small_loads:
        copy.wait()
    place = lax.broadcasted_iota(jnp.int32, (channels, columns), 1)
    weight = jnp.where(place < count_ref[0], obs_weight_ref[...], 0.0)
    weight_high = weight.astype(jnp.bfloat16)
    jac_vmem[layers] = weight_high
    jac_vmem[layers + 1] = (weight - weight_high.astype(jnp.float32)).astype(jnp.bfloat16)
    scaled = (weight * depart_ref[...]).astype(jnp.bfloat16).astype(jnp.float32)
    for copies in loads:
        for copy in copies:
            copy.wait()

    def source_rows(first, count):
        block = jac_vmem[pl.ds(first, count)].astype(jnp.float32)
        source_ref[pl.ds(first, count)] = jnp.sum(block * scaled[None], axis=1)

    def source_step(q, carry):
        source_rows(q * SUB, SUB)
        return carry

    with scope("source"):
        lax.fori_loop(0, layers // SUB, source_step, 0)
    source_rows(layers // SUB * SUB, layers % SUB)
    mixed_ref[...] = jnp.zeros((channels, columns), jnp.float32)
    for k in range(block_count):
        mixed_ref[0:1, k * BLOCK : (k + 1) * BLOCK] = jnp.full((1, BLOCK), block_ref[k].astype(jnp.float32))
    mixed_ref[1 : 1 + layers - LANES] = source_ref[LANES:layers]
    jac_vmem[layers + 2] = mixed_ref[...].astype(jnp.bfloat16)
    source_slots = LANES // channels
    for q in range(source_slots):
        jac_vmem[layers + 3 + q] = source_ref[q * channels : (q + 1) * channels].astype(jnp.bfloat16)
    for extra in range(layers + 3 + source_slots, padded):
        jac_vmem[extra] = jnp.zeros((channels, columns), jnp.bfloat16)

    def one_hot(shape, wanted):
        row = lax.broadcasted_iota(jnp.int32, shape, 0)
        column = lax.broadcasted_iota(jnp.int32, shape, 1)
        return jnp.where(column == wanted(row), 1.0, 0.0).astype(jnp.bfloat16)

    order_ref[...] = one_hot(
        (columns, columns), lambda r: r % mine // SUB * BLOCK + r // mine * SUB + r % SUB
    )
    width = SUB * channels
    back_order_ref[...] = one_hot((width, width), lambda r: r % SUB * channels + r // SUB)

    def stage(p):
        for i, chunk in enumerate(pieces[p]):
            block = jac_vmem[chunk * SUB : (chunk + 1) * SUB].reshape(width, columns)
            turned = one_hot_dot(order_ref[...], block).astype(jnp.bfloat16)
            put_ref[p, :, i] = turned.reshape(group, mine, width)

    def send(p):
        def one(k, carry):
            member = other(k)
            pltpu.make_async_remote_copy(
                src_ref=put_ref.at[p, member],
                dst_ref=got_ref.at[p, slot],
                send_sem=jac_send.at[p],
                recv_sem=jac_recv.at[p],
                device_id=coords(member),
                device_id_type=MESH,
            ).start()
            return carry

        lax.fori_loop(1, group, one, 0)
        got_ref[p, slot] = put_ref[p, me]

    with scope("stage0"):
        stage(0)
    with scope("barrier"):
        pl.semaphore_wait(barrier, group)
    with scope("sends"):
        for p in range(piece_count):
            if p:
                stage(p)
            send(p)

    cov = cov_ref[...]
    rest = layers - LANES
    gram_ref[...] = jnp.zeros(gram_ref.shape, jnp.float32)
    out_maps_ref[...] = jnp.zeros(out_maps_ref.shape, jnp.float32)
    gram = exact_dot(cov, cov, TN)
    gram_ref[0:layers, 0:layers] = gram
    out_maps_ref[0, 0:layers, 0:layers] = gram
    same = lax.broadcasted_iota(jnp.int32, cov.shape, 0) == lax.broadcasted_iota(jnp.int32, cov.shape, 1)
    turned_cov = exact_dot(jnp.where(same, 1.0, 0.0), cov, NT)
    out_maps_ref[1, 0:layers, 0:LANES] = turned_cov[:, :LANES]
    out_maps_ref[1, 0:layers, LANES + 2 * SUB : LANES + 2 * SUB + rest] = turned_cov[:, LANES:]

    def take(p):
        others = got_ref.at[p, pl.ds(0, group - 1)]
        pltpu.make_async_copy(others, others, jac_recv.at[p]).wait()
        for i, chunk in enumerate(pieces[p]):
            block = got_ref[p, :, i].reshape(group * mine, width)
            turned = one_hot_dot(back_order_ref[...], block)
            for low in range(lows):
                part = turned[:, low * LANES : (low + 1) * LANES].reshape(channels, SUB, LANES)
                kernel_ref[low * channels : (low + 1) * channels, chunk * SUB : (chunk + 1) * SUB, :] = part

    half_rows = padded // 2
    lane = lax.broadcasted_iota(jnp.int32, (half_rows, LANES), 1)

    def terms_copy(step):
        return pltpu.make_async_remote_copy(
            src_ref=terms_ref.at[step, 0], dst_ref=terms_ref.at[step, 1],
            send_sem=term_send.at[step], recv_sem=term_recv.at[step],
            device_id=partner, device_id_type=MESH,
        )

    def put_terms(step, terms):
        summed = terms + pltpu.roll(terms, LANES // 2, 1)
        packed = jnp.where(lane < LANES // 2, summed[:half_rows], summed[half_rows:])
        terms_ref[step, 0] = packed
        terms_copy(step).start()

    with scope("take0"):
        take(0)
    weight_ref[...] = kernel_ref[:, layers, :] + kernel_ref[:, layers + 1, :]
    id_ref[0] = jnp.broadcast_to(kernel_ref[0, layers + 2 : layers + 3, :], (SUB, LANES))
    id_copy = pltpu.make_async_remote_copy(
        src_ref=id_ref.at[0], dst_ref=id_ref.at[1], send_sem=id_send, recv_sem=id_recv,
        device_id=partner, device_id_type=MESH,
    )
    id_copy.start()

    def low_sum(first, count, layer):
        return sum(
            kernel_ref[low * channels + first : low * channels + first + count, layer, :] for low in range(lows)
        )

    for q in range(source_slots):
        spread_ref[q * channels : (q + 1) * channels] = low_sum(0, channels, layers + 3 + q)
    spread_ref[LANES:padded] = jnp.zeros((padded - LANES, LANES), jnp.float32)
    spread_ref[LANES:layers] = low_sum(1, layers - LANES, layers + 2)
    put_terms(0, spread_ref[...])
    early = piece_count - 2
    with scope("takes"):
        for p in range(1, early):
            take(p)

    with scope("idwait"):
        id_copy.wait()
    grid_row = lax.broadcasted_iota(jnp.int32, (LANES, LANES), 0)
    grid_lane = lax.broadcasted_iota(jnp.int32, (LANES, LANES), 1)

    def pick_of(which):
        wanted = id_ref[which, 0:1, :].astype(jnp.int32) * SUB + grid_lane % SUB
        return jnp.where(grid_row == wanted, 1.0, 0.0).astype(jnp.bfloat16)

    own_pick = pick_of(0)
    both_picks = jnp.concatenate([own_pick, pick_of(1)], axis=1)
    matched = one_hot_dot(own_pick, both_picks, TN).astype(jnp.bfloat16)
    relation = jnp.concatenate([both_picks, matched], axis=0).astype(jnp.float32)
    relation_lane = lax.broadcasted_iota(jnp.int32, relation.shape, 1) % LANES
    for which in range(2):
        kept = relation_lane // (LANES // 2) == which
        relation_ref[which] = jnp.where(kept, relation, 0.0).astype(jnp.bfloat16)

    zero = jnp.zeros((padded, LANES), jnp.float32)

    def collected(step):
        with scope("waitterms"):
            terms_copy(step).wait()
        both = jnp.concatenate([terms_ref[step, 0], terms_ref[step, 1]], axis=1)
        high = both.astype(jnp.bfloat16)
        low = (both - high.astype(jnp.float32)).astype(jnp.bfloat16)
        parts = jnp.concatenate([high.astype(jnp.float32), low.astype(jnp.float32)], axis=0).astype(jnp.bfloat16)
        sums = [one_hot_dot(parts, relation_ref[which]) for which in range(2)]
        return jnp.concatenate([value[:half_rows] + value[half_rows:] for value in sums], axis=0)

    def put_normal(step, spread, with_square=False):
        def normal_step(n, carry):
            acc, square = carry
            kernel = kernel_ref[n]
            predicted = jnp.sum(kernel * spread, axis=0, keepdims=True)
            scaled = predicted * weight_ref[pl.ds(n, 1), :]
            if with_square:
                square = square + predicted * scaled
            return acc + kernel * scaled, square

        acc, square = lax.fori_loop(0, rows, normal_step, (zero, zero[:1]), unroll=4)
        put_terms(step, acc)
        return square

    def gram_dot(field):
        return exact_dot(gram_ref[...], field, (((1,), (0,)), ((), ())))

    def row_of(a, b):
        return jnp.sum(a * b, axis=0, keepdims=True)

    residual_both = collected(0)
    spread_both = gram_dot(residual_both)
    residual, spread = residual_both[:, :LANES], spread_both[:, :LANES]
    spread_ref[...] = spread_both[:, LANES:]

    def predict(p, begin):
        def predict_step(n, carry):
            total = None if begin else predicted_ref[n]
            for chunk in pieces[p]:
                part = pl.ds(chunk * SUB, SUB)
                product = kernel_ref[n, part, :] * spread_ref[part, :]
                total = product if total is None else total + product
            predicted_ref[n] = total
            return carry

        lax.fori_loop(0, rows, predict_step, 0, unroll=8)

    with scope("predict"):
        for p in range(early):
            predict(p, p == 0)
    with scope("takelast"):
        for p in range(early, piece_count):
            take(p)
            predict(p, False)

    def adjoint_step(n, acc):
        scaled = jnp.sum(predicted_ref[n], axis=0, keepdims=True) * weight_ref[pl.ds(n, 1), :]
        return acc + kernel_ref[n] * scaled

    with scope("adjoint1"):
        put_terms(1, lax.fori_loop(0, rows, adjoint_step, zero, unroll=4))
    with scope("collect1"):
        applied_both = residual_both + collected(1)

    def share_row(ref, send_sem, recv_sem, place, targets):
        copies = [
            pltpu.make_async_remote_copy(
                src_ref=ref.at[place], dst_ref=ref.at[place], send_sem=send_sem, recv_sem=recv_sem,
                device_id=target, device_id_type=MESH,
            )
            for target in targets
        ]
        for copy in copies:
            copy.start()

    def wait_rows(ref, send_sem, recv_sem, count):
        others = ref.at[pl.ds(0, count)]
        pltpu.make_async_copy(others, others, recv_sem).wait()
        pltpu.make_async_copy(others, others, send_sem).wait()

    group_targets = [coords(other(k)) for k in range(1, group)]
    control = direction = image = spread_image = image_applied = None
    norm_last = step_last = None
    for step in range(ITERS - 2):
        applied = applied_both[:, :LANES]
        parts_ref[step, me, 0:1] = row_of(residual, spread)
        parts_ref[step, me, 1:2] = row_of(applied, spread)
        with scope("sendsum"):
            share_row(parts_ref.at[step], sum_send.at[step], sum_recv.at[step], me, group_targets)
        with scope("normal"):
            next_spread = gram_dot(applied_both)
            put_normal(step + 2, next_spread[:, LANES:])
        with scope("waitsum"):
            wait_rows(parts_ref.at[step], sum_send.at[step], sum_recv.at[step], group - 1)
        total = jnp.sum(parts_ref[step], axis=0)
        total = jnp.sum(total, axis=1, keepdims=True)
        norm_now, curve = total[0:1], total[1:2]
        if step == 0:
            length = norm_now / curve
            direction, image = residual, applied
            control = length * direction
        else:
            ratio = norm_now / norm_last
            length = norm_now / (curve - ratio * norm_now / step_last)
            direction = residual + ratio * direction
            image = applied + ratio * image
            control = control + length * direction
        residual = residual - length * image
        if step == 0:
            spread_image = next_spread[:, :LANES]
            image_applied = applied_both + collected(step + 2)
        else:
            spread_image = next_spread[:, :LANES] + ratio * spread_image
            image_applied = applied_both + collected(step + 2) + ratio * image_applied
        spread = spread - length * spread_image
        applied_both = applied_both - length * image_applied
        norm_last, step_last = norm_now, length

    applied, image_applied = applied_both[:, :LANES], image_applied[:, :LANES]
    with scope("normal"):
        next_spread_both = gram_dot(applied_both)
        square = put_normal(ITERS, next_spread_both[:, LANES:], True)
    next_spread = next_spread_both[:, :LANES]
    pairs = (
        (residual, spread), (applied, spread), (image, spread), (applied, next_spread),
        (image, next_spread), (image, spread_image), (image_applied, next_spread), (image_applied, spread_image),
    )
    wide = [row_of(a, b) * 0.5 for a, b in pairs] + [square]
    spot = lax.broadcasted_iota(jnp.int32, (1, LANES), 1)
    row = jnp.zeros((1, LANES), jnp.float32)
    for i, value in enumerate(wide):
        row = jnp.where(spot == i, jnp.sum(value, axis=1, keepdims=True), row)
    finals_ref[rank] = row
    with scope("sendsum"):
        share_row(finals_ref, final_send, final_recv, rank, [any_other(k) for k in range(1, device_count)])
    with scope("waitsum"):
        wait_rows(finals_ref, final_send, final_recv, device_count - 1)
    total = jnp.sum(finals_ref[...], axis=0)
    sums = [jnp.sum(jnp.where(spot == i, total, 0.0), axis=1, keepdims=True) for i in range(len(wide))]
    norm_now, curve, rest_image, next_next, image_next, image_image, twice_next, twice_image, square = sums
    ratio = norm_now / norm_last
    length = norm_now / (curve - ratio * norm_now / step_last)
    along = curve + ratio * rest_image
    image_square = next_next + ratio * (2.0 * image_next + ratio * image_image)
    norm_next = norm_now - length * (2.0 * along - length * image_square)
    cross = next_next + ratio * image_next
    image_curve = next_next + square + ratio * (2.0 * twice_next + ratio * twice_image)
    curve_next = curve - length * (2.0 * cross - length * image_curve)
    ratio_next = norm_next / norm_now
    length_next = norm_next / (curve_next - ratio_next * norm_next / length)
    direction = residual + ratio * direction
    image = applied + ratio * image
    control = control + length * direction
    residual = residual - length * image
    control = control + length_next * (residual + ratio_next * direction)
    applied = applied - length * (applied + collected(ITERS)[:, :LANES] + ratio * image_applied)
    residual = residual - length_next * (applied + ratio_next * image)

    outs = [exact_dot(value, out_maps_ref[which], TN) for which, value in enumerate((control, residual))]
    staged = [outs[0][:, :LANES], outs[1][:, :LANES], outs[0][:, LANES:] + outs[1][:, LANES:]]
    for which, value in enumerate(staged):
        value = value.astype(jnp.bfloat16).reshape(obs_count, GRID_BLK, SUB, LANES)
        back_ref[0, 0:obs_count, :, :, which * LANES : (which + 1) * LANES] = value

    def back_source(member):
        return back_ref.at[0, top * half_obs + member // chan_count]

    def send_back(k, carry):
        member = other(k)
        pltpu.make_async_remote_copy(
            src_ref=back_source(member),
            dst_ref=back_ref.at[1, me],
            send_sem=back_send,
            recv_sem=back_recv,
            device_id=coords(member),
            device_id_type=MESH,
        ).start()
        return carry

    with scope("sendback"):
        lax.fori_loop(1, group, send_back, 0)
    back_ref[1, me] = back_ref[0, obs]
    for p in range(piece_count):
        others = put_ref.at[p, pl.ds(0, group - 1)]
        pltpu.make_async_copy(others, others, jac_send.at[p]).wait()
    others = back_ref.at[1, pl.ds(0, group - 1)]
    with scope("waitback"):
        pltpu.make_async_copy(others, others, back_recv).wait()
    pltpu.make_async_copy(others, others, back_send).wait()
    straight = one_hot((LANES, LANES), lambda r: r)
    for block in range(GRID_BLK):
        spots = slice(block * BLOCK, (block + 1) * BLOCK)
        turned = [
            one_hot_dot(straight, back_ref[1, :, block, :, i * LANES : (i + 1) * LANES].reshape(group * SUB, LANES))
            for i in range(3)
        ]
        for which, out_ref in enumerate((increment_ref, residual_ref)):
            out_ref[0:LANES, spots] = turned[which].astype(jnp.bfloat16)
            first = which * 2 * SUB
            out_ref[LANES:layers, spots] = turned[2][first : first + layers - LANES].astype(jnp.bfloat16)


def half_slice_columns(jacobian, departures, obs_weights, column_count, grid_block, sqrt_cov):
    obs_count, chan_count = lax.axis_size("obs"), lax.axis_size("chan")
    group = obs_count // 2 * chan_count
    capacity, channels, layers = jacobian.shape
    mine = capacity // BLOCK * SUB
    padded = LANES + 2 * SUB
    chunk_count = padded // SUB
    piece_count = chunk_count // PIECE
    rows = channels * chan_count // 2
    width = SUB * channels

    out = pltpu.VMEM((layers, GRID_BLK * BLOCK), jnp.bfloat16)
    hbm = pl.BlockSpec(memory_space=pltpu.HBM)
    vmem = pl.BlockSpec(memory_space=pltpu.VMEM)
    dma = pltpu.SemaphoreType.DMA
    bf16, f32 = jnp.bfloat16, jnp.float32
    increment, residual = pl.pallas_call(
        functools.partial(cg_kernel, obs_count, chan_count),
        out_shape=(out, out),
        in_specs=[hbm] * 6,
        out_specs=(vmem, vmem),
        scratch_shapes=[
            pltpu.VMEM(obs_weights.shape, f32),
            pltpu.VMEM(departures.shape, f32),
            pltpu.SMEM(column_count.shape, jnp.int32),
            pltpu.SMEM(grid_block.shape, jnp.int32),
            pltpu.VMEM(sqrt_cov.shape, f32),
            pltpu.VMEM((padded, channels, capacity), bf16),
            pltpu.VMEM((padded, capacity), f32),
            pltpu.VMEM((channels, capacity), f32),
            pltpu.VMEM((piece_count, group, PIECE, mine, width), bf16),
            pltpu.VMEM((piece_count, group, PIECE, mine, width), bf16),
            pltpu.VMEM((rows, padded, LANES), f32),
            pltpu.VMEM((rows, LANES), f32),
            pltpu.VMEM((capacity, capacity), bf16),
            pltpu.VMEM((width, width), bf16),
            pltpu.VMEM((padded, padded), f32),
            pltpu.VMEM((2, padded, 2 * LANES), f32),
            pltpu.VMEM((padded, LANES), f32),
            pltpu.VMEM((rows, SUB, LANES), f32),
            pltpu.VMEM((2, 2 * LANES, 2 * LANES), bf16),
            pltpu.VMEM((2, SUB, LANES), f32),
            pltpu.VMEM((STEPS, 2, padded // 2, LANES), f32),
            pltpu.VMEM((ITERS - 2, group, 2, LANES), f32),
            pltpu.VMEM((obs_count * chan_count, 1, LANES), f32),
            pltpu.VMEM((2, group, GRID_BLK, SUB, 3 * LANES), bf16),
            dma((5,)), dma((piece_count + 1,)),
            dma((piece_count,)), dma((piece_count,)),
            dma, dma,
            dma((STEPS,)), dma((STEPS,)),
            dma((ITERS - 2,)), dma((ITERS - 2,)),
            dma, dma,
            dma, dma,
        ],
        compiler_params=pltpu.CompilerParams(
            collective_id=0, has_side_effects=True, vmem_limit_bytes=VMEM_BYTES
        ),
    )(jacobian.transpose(2, 1, 0), obs_weights, departures, column_count, grid_block, sqrt_cov)
    return increment.T.astype(f32), residual.T.astype(f32)


def solution(mesh):
    obs_count, chan_count = mesh.shape["obs"], mesh.shape["chan"]
    group = obs_count // 2 * chan_count

    def plan(jacobian, departures, obs_weights, column_count, grid_block, sqrt_cov):
        capacity, channels, layers = jacobian.shape
        mine = capacity // BLOCK * SUB
        fits = (
            obs_count % 2 == 0
            and chan_count % 2 == 0
            and group * SUB == BLOCK
            and obs_count * mine == LANES
            and obs_count * GRID_BLK * SUB == LANES
            and chan_count == 4
            and channels == 32
            and LANES + SUB < layers <= LANES + 2 * SUB - 7
        )
        chosen = half_slice_columns if fits else exchange_per_step
        return chosen(jacobian, departures, obs_weights, column_count, grid_block, sqrt_cov)

    in_specs = (P("obs", "chan", None), P("chan", "obs"), P("chan", "obs"), P("obs"), P("obs"), P())
    out_specs = (P("obs", None), P("obs", None))
    return jax.shard_map(plan, mesh=mesh, in_specs=in_specs, out_specs=out_specs, check_vma=False)
```

```python
import contextlib
import functools
import jax
import jax.numpy as jnp
from jax import lax
from jax.experimental import pallas as pl
from jax.experimental.pallas import tpu as pltpu
from jax.sharding import PartitionSpec as P

BLOCK = 128
ITERS = 5
GRID_BLK = 2
HIGHEST = lax.Precision.HIGHEST
MESH = pl.DeviceIdType.MESH


def block_terms(jac_part, weight_part, mask_part, predicted):
    scaled = (mask_part[:, None] * weight_part * predicted).astype(jnp.bfloat16)
    return lax.dot_general(
        jac_part, scaled, (((1,), (1,)), ((0,), (0,))), preferred_element_type=jnp.float32
    )


def forward_terms(jac_part, weight_part, mask_part, field_part):
    predicted = lax.dot_general(
        jac_part, field_part, (((2,), (1,)), ((0,), (0,))), preferred_element_type=jnp.float32
    )
    return block_terms(jac_part, weight_part, mask_part, predicted)


def exchange_per_step(jacobian, departures, obs_weights, column_count, grid_block, sqrt_cov):
    obs_count = lax.axis_size("obs")
    myself = lax.axis_index("obs")
    capacity, group_channels, layers = jacobian.shape
    block_count = capacity // BLOCK
    weight_cols = obs_weights.T
    depart_cols = departures.T
    observed = (jnp.arange(capacity, dtype=jnp.int32) < column_count[0]).astype(jnp.float32)
    every_id = lax.all_gather(grid_block, "obs", axis=0, tiled=True).reshape(obs_count, block_count)
    targets = jnp.arange(obs_count, dtype=jnp.int32)
    send_pick = (grid_block[None, :] // GRID_BLK == targets[:, None]).astype(jnp.float32)
    owned_here = every_id // GRID_BLK == myself
    places = every_id % GRID_BLK
    grid_index = jnp.arange(GRID_BLK, dtype=jnp.int32)
    take_pick = jnp.sum(
        ((places[None] == grid_index[:, None, None]) & owned_here[None]).astype(jnp.float32), axis=2
    )
    share_cols = BLOCK

    def local_terms(kernel_fn, inputs):
        return kernel_fn(jacobian, weight_cols, observed, inputs)

    def to_owners(terms):
        blocked = terms.reshape(block_count, BLOCK, layers)
        blocked = lax.psum(blocked, "chan")
        outgoing = jnp.dot(
            send_pick, blocked.reshape(block_count, -1), precision=lax.Precision.HIGHEST
        )
        incoming = lax.all_to_all(
            outgoing.reshape(obs_count, share_cols, layers),
            "obs",
            split_axis=0,
            concat_axis=0,
            tiled=True,
        )
        summed = jnp.dot(
            take_pick, incoming.reshape(obs_count, -1), precision=lax.Precision.HIGHEST
        )
        return summed.reshape(GRID_BLK, share_cols, layers)

    def spread(field):
        return jnp.dot(
            field.reshape(-1, layers), sqrt_cov, precision=lax.Precision.HIGHEST
        ).reshape(field.shape)

    def spread_back(field):
        flat = lax.dot_general(
            field.reshape(-1, layers),
            sqrt_cov,
            (((1,), (1,)), ((), ())),
            precision=lax.Precision.HIGHEST,
        )
        return flat.reshape(field.shape)

    def squared(values):
        partial_sum = jnp.sum(values * values)
        return lax.psum(partial_sum, "obs")

    residual = spread_back(to_owners(local_terms(block_terms, depart_cols)))
    control = jnp.zeros_like(residual)
    direction = residual
    norm_now = squared(residual)
    for iteration in range(ITERS):
        rounded = spread(direction).astype(jnp.bfloat16).reshape(GRID_BLK, -1)
        to_outgoing = jnp.dot(
            take_pick.T.astype(jnp.bfloat16), rounded, preferred_element_type=jnp.float32
        ).astype(jnp.bfloat16)
        to_incoming = lax.all_to_all(
            to_outgoing.reshape(obs_count, share_cols, layers),
            "obs",
            split_axis=0,
            concat_axis=0,
            tiled=True,
        )
        picked = jnp.dot(
            send_pick.T.astype(jnp.bfloat16),
            to_incoming.reshape(obs_count, -1),
            preferred_element_type=jnp.float32,
        )
        picked = picked.astype(jnp.bfloat16).reshape(block_count, share_cols, layers)
        fetched = picked.reshape(capacity, layers)
        image = direction + spread_back(to_owners(local_terms(forward_terms, fetched)))
        curvature_partial_sum = jnp.sum(direction * image)
        step_length = norm_now / lax.psum(curvature_partial_sum, "obs")
        control = control + step_length * direction
        residual = residual - step_length * image
        norm_next = squared(residual)
        direction = residual + norm_next / norm_now * direction
        norm_now = norm_next
    increment = spread(control)
    return (increment.reshape(-1, layers), residual.reshape(-1, layers))


LANES = 128
SUB = 8
LEVELS = 32000.0
PIECES = (1, 3, 3, 4, 4, 2, 1)
AHEAD = 3
LATE = 2
LOADS = 4
VMEM_BYTES = 67043328 - 1024 * 1024
STEPS = ITERS + 1
scope = lambda name: contextlib.nullcontext()
NT = (((1,), (1,)), ((), ()))
TN = (((0,), (0,)), ((), ()))


def exact_dot(a, b, dims):
    return lax.dot_general(a, b, dims, precision=HIGHEST, preferred_element_type=jnp.float32)


def one_hot_dot(a, b, dims=NT):
    return lax.dot_general(a, b, dims, preferred_element_type=jnp.float32)


def cg_kernel(
    obs_count, chan_count, jac_ref, *rest
):
    smalls, (increment_ref, residual_ref), rest = rest[:5], rest[5:7], rest[7:]
    run_cg(obs_count, chan_count, jac_ref, smalls, rest[:5], increment_ref, residual_ref, *rest[5:])


def run_cg(
    obs_count, chan_count, jac_ref, small_hbm, small_refs, increment_ref, residual_ref,
    jac_vmem, source_ref, mixed_ref, put_ref, got_ref, kernel_ref, weight_ref, order_ref, back_order_ref,
    gram_ref, gram_parts_ref, cov_pad_ref, cov_parts_ref, spread_ref, predicted_ref, scaled_ref, relation_ref, id_ref, terms_ref, scale_ref, parts_ref, finals_ref, back_ref,
    small_sem, load_sem, jac_send, jac_recv, id_send, id_recv, term_send, term_recv, sum_send, sum_recv,
    final_send, final_recv, back_send, back_recv
):
    obs_weight_ref, depart_ref, count_ref, block_ref, cov_ref = small_refs
    small_loads = [
        pltpu.make_async_copy(source, target, small_sem.at[i])
        for i, (source, target) in enumerate(zip(small_hbm, small_refs))
    ]
    for copy in small_loads:
        copy.start()
    layers, channels, columns = jac_ref.shape
    padded = jac_vmem.shape[0]
    bounds = [layers // SUB * (i + 1) // LOADS * SUB for i in range(LOADS - 1)]
    bounds = list(zip([0] + bounds, bounds + [layers]))
    loads = [
        pltpu.make_async_copy(jac_ref.at[pl.ds(a, b - a)], jac_vmem.at[pl.ds(a, b - a)], load_sem.at[i])
        for i, (a, b) in enumerate(bounds)
    ]
    for copy in loads:
        copy.start()
    chunk_count = padded // SUB
    piece_count = len(PIECES)
    half_obs = obs_count // 2
    group = half_obs * chan_count
    rows = kernel_ref.shape[0]
    lows = chan_count // 2
    block_count = columns // BLOCK
    mine = block_count * SUB

    obs, chan = lax.axis_index("obs"), lax.axis_index("chan")
    top = obs // half_obs
    me = (obs % half_obs) * chan_count + chan
    slot = (chan % lows) * (2 * half_obs) + (chan // lows) * half_obs + obs % half_obs

    def coords(member):
        return (top * half_obs + member // chan_count, member % chan_count)

    def other(k):
        member, place = 0, 1
        while place < group:
            member = member + (me // place + k // place) % 2 * place
            place *= 2
        return member

    device_count = obs_count * chan_count
    rank = obs * chan_count + chan

    def any_other(k):
        member, place = 0, 1
        while place < device_count:
            member = member + (rank // place + k // place) % 2 * place
            place *= 2
        return (member // chan_count, member % chan_count)

    partner = ((obs + half_obs) % obs_count, chan)
    barrier = pltpu.get_barrier_semaphore()

    def greet(k, carry):
        pl.semaphore_signal(barrier, inc=1, device_id=coords(other(k)), device_id_type=MESH)
        return carry

    lax.fori_loop(1, group, greet, 0)
    pl.semaphore_signal(barrier, inc=1, device_id=partner, device_id_type=MESH)

    chunks = [chunk_count - 1] + list(range(chunk_count - 1))
    starts = [sum(PIECES[:p]) for p in range(piece_count)]
    def one_hot(shape, wanted):
        row = lax.broadcasted_iota(jnp.int32, shape, 0)
        column = lax.broadcasted_iota(jnp.int32, shape, 1)
        return jnp.where(column == wanted(row), 1.0, 0.0).astype(jnp.bfloat16)

    order_ref[...] = one_hot(
        (columns, columns), lambda r: r % mine // SUB * BLOCK + r // mine * SUB + r % SUB
    )
    width = SUB * channels
    back_order_ref[...] = one_hot((width, width), lambda r: r % SUB * channels + r // SUB)

    with scope("smallwait"):
        for copy in small_loads:
            copy.wait()
    place = lax.broadcasted_iota(jnp.int32, (channels, columns), 1)
    weight = jnp.where(place < count_ref[0], obs_weight_ref[...], 0.0)
    weight_high = weight.astype(jnp.bfloat16)
    jac_vmem[layers] = weight_high
    jac_vmem[layers + 1] = (weight - weight_high.astype(jnp.float32)).astype(jnp.bfloat16)
    scaled = (weight * depart_ref[...]).astype(jnp.bfloat16).astype(jnp.float32)

    def source_rows(first, count):
        block = jac_vmem[pl.ds(first, count)].astype(jnp.float32)
        source_ref[pl.ds(first, count)] = jnp.sum(block * scaled[None], axis=1)

    def source_step(q, carry):
        source_rows(q * SUB, SUB)
        return carry

    for copy, (a, b) in zip(loads, bounds):
        with scope("loadwait"):
            copy.wait()
        with scope("source"):
            lax.fori_loop(a // SUB, b // SUB, source_step, 0)
    source_rows(layers // SUB * SUB, layers % SUB)
    mixed_ref[...] = jnp.zeros((channels, columns), jnp.float32)
    for k in range(block_count):
        mixed_ref[0:1, k * BLOCK : (k + 1) * BLOCK] = jnp.full((1, BLOCK), block_ref[k].astype(jnp.float32))
    mixed_ref[1 : 1 + layers - LANES] = source_ref[LANES:layers]
    jac_vmem[layers + 2] = mixed_ref[...].astype(jnp.bfloat16)
    source_slots = LANES // channels
    for q in range(source_slots):
        jac_vmem[layers + 3 + q] = source_ref[q * channels : (q + 1) * channels].astype(jnp.bfloat16)
    for extra in range(layers + 3 + source_slots, padded):
        jac_vmem[extra] = jnp.zeros((channels, columns), jnp.bfloat16)

    def span(p):
        return pl.ds(starts[p], PIECES[p])

    def chunks_of(p):
        return [(i, chunks[i]) for i in range(starts[p], starts[p] + PIECES[p])]

    def stage(p):
        for i, chunk in chunks_of(p):
            block = jac_vmem[chunk * SUB : (chunk + 1) * SUB].reshape(width, columns)
            turned = one_hot_dot(order_ref[...], block).astype(jnp.bfloat16)
            put_ref[:, i] = turned.reshape(group, mine, width)

    def send(p):
        def one(k, carry):
            member = other(k)
            pltpu.make_async_remote_copy(
                src_ref=put_ref.at[member, span(p)],
                dst_ref=got_ref.at[slot, span(p)],
                send_sem=jac_send.at[p],
                recv_sem=jac_recv.at[p],
                device_id=coords(member),
                device_id_type=MESH,
            ).start()
            return carry

        lax.fori_loop(1, group, one, 0)
        for i, _ in chunks_of(p):
            got_ref[slot, i] = put_ref[me, i]

    with scope("stage0"):
        stage(0)
    with scope("barrier"):
        pl.semaphore_wait(barrier, group)
    with scope("sends"):
        for p in range(AHEAD):
            if p:
                stage(p)
            send(p)
        for p in range(AHEAD, piece_count):
            stage(p)

    cov = cov_ref[...]
    gram_ref[...] = jnp.zeros(gram_ref.shape, jnp.float32)
    cov_pad_ref[...] = jnp.zeros(cov_pad_ref.shape, jnp.float32)
    gram = exact_dot(cov, cov, TN)
    gram_ref[0:layers, 0:layers] = gram
    gram_high = gram_ref[...].astype(jnp.bfloat16)
    gram_low = (gram_ref[...] - gram_high.astype(jnp.float32)).astype(jnp.bfloat16)
    gram_parts_ref[...] = jnp.concatenate([gram_high, gram_high, gram_low], axis=1)
    cov_pad_ref[0:layers, 0:layers] = cov
    cov_high = cov_pad_ref[...].astype(jnp.bfloat16)
    cov_low = (cov_pad_ref[...] - cov_high.astype(jnp.float32)).astype(jnp.bfloat16)
    cov_parts_ref[...] = jnp.concatenate([cov_high, cov_high, cov_low], axis=1)

    def take(p):
        others = got_ref.at[pl.ds(0, group - 1), span(p)]
        pltpu.make_async_copy(others, others, jac_recv.at[p]).wait()
        for i, chunk in chunks_of(p):
            block = got_ref[:, i].reshape(group * mine, width)
            turned = one_hot_dot(back_order_ref[...], block)
            for low in range(lows):
                part = turned[:, low * LANES : (low + 1) * LANES].reshape(channels, SUB, LANES)
                kernel_ref[low * channels : (low + 1) * channels, chunk * SUB : (chunk + 1) * SUB, :] = part

    half_rows = padded // 2
    lane = lax.broadcasted_iota(jnp.int32, (half_rows, LANES), 1)

    def terms_copies(step):
        return [
            pltpu.make_async_remote_copy(
                src_ref=ref.at[step, 0], dst_ref=ref.at[step, 1],
                send_sem=term_send.at[step, i], recv_sem=term_recv.at[step, i],
                device_id=partner, device_id_type=MESH,
            )
            for i, ref in enumerate((scale_ref, terms_ref))
        ]

    def put_terms(step, terms):
        summed = terms + pltpu.roll(terms, LANES // 2, 1)
        packed = jnp.where(lane < LANES // 2, summed[:half_rows], summed[half_rows:])
        largest = jnp.maximum(jnp.max(jnp.abs(packed), axis=0, keepdims=True), 1e-30)
        scale_ref[step, 0] = largest * (1.0 / LEVELS)
        terms_ref[step, 0] = jnp.round(packed * (LEVELS / largest)).astype(jnp.int32).astype(jnp.int16)
        for copy in terms_copies(step):
            copy.start()

    with scope("take0"):
        take(0)
    weight_ref[...] = kernel_ref[:, layers, :] + kernel_ref[:, layers + 1, :]
    id_ref[0] = jnp.broadcast_to(kernel_ref[0, layers + 2 : layers + 3, :], (SUB, LANES))
    id_copy = pltpu.make_async_remote_copy(
        src_ref=id_ref.at[0], dst_ref=id_ref.at[1], send_sem=id_send, recv_sem=id_recv,
        device_id=partner, device_id_type=MESH,
    )
    id_copy.start()

    def low_sum(first, count, layer):
        return sum(
            kernel_ref[low * channels + first : low * channels + first + count, layer, :] for low in range(lows)
        )

    for q in range(source_slots):
        spread_ref[q * channels : (q + 1) * channels] = low_sum(0, channels, layers + 3 + q)
    spread_ref[LANES:padded] = jnp.zeros((padded - LANES, LANES), jnp.float32)
    spread_ref[LANES:layers] = low_sum(1, layers - LANES, layers + 2)
    put_terms(0, spread_ref[...])
    with scope("sends2"):
        for p in range(AHEAD, piece_count):
            send(p)
    early = piece_count - LATE
    with scope("takes"):
        for p in range(1, early):
            take(p)

    with scope("idwait"):
        id_copy.wait()
    grid_row = lax.broadcasted_iota(jnp.int32, (LANES, LANES), 0)
    grid_lane = lax.broadcasted_iota(jnp.int32, (LANES, LANES), 1)

    def pick_of(which):
        wanted = id_ref[which, 0:1, :].astype(jnp.int32) * SUB + grid_lane % SUB
        return jnp.where(grid_row == wanted, 1.0, 0.0).astype(jnp.bfloat16)

    own_pick = pick_of(0)
    both_picks = jnp.concatenate([own_pick, pick_of(1)], axis=1)
    matched = one_hot_dot(own_pick, both_picks, TN).astype(jnp.bfloat16)
    relation = jnp.concatenate([both_picks, matched], axis=0).astype(jnp.float32)
    relation_lane = lax.broadcasted_iota(jnp.int32, relation.shape, 1) % LANES
    for which in range(2):
        kept = relation_lane // (LANES // 2) == which
        relation_ref[which] = jnp.where(kept, relation, 0.0).astype(jnp.bfloat16)

    zero = jnp.zeros((padded, LANES), jnp.float32)

    def collected(step):
        with scope("waitterms"):
            for copy in terms_copies(step):
                copy.wait()
        both = [terms_ref[step, i].astype(jnp.int32).astype(jnp.float32) * scale_ref[step, i] for i in range(2)]
        both = jnp.concatenate(both, axis=1)
        high = both.astype(jnp.bfloat16)
        low = (both - high.astype(jnp.float32)).astype(jnp.bfloat16)
        parts = jnp.concatenate([high.astype(jnp.float32), low.astype(jnp.float32)], axis=0).astype(jnp.bfloat16)
        sums = [one_hot_dot(parts, relation_ref[which]) for which in range(2)]
        return jnp.concatenate([value[:half_rows] + value[half_rows:] for value in sums], axis=0)

    def put_normal(step, spread):
        def normal_step(n, acc):
            kernel = kernel_ref[n]
            predicted = jnp.sum(kernel * spread, axis=0, keepdims=True)
            return acc + kernel * (predicted * weight_ref[pl.ds(n, 1), :])

        put_terms(step, lax.fori_loop(0, rows, normal_step, zero, unroll=4))

    def predict_all(spread):
        def predict_step(n, square):
            predicted = jnp.sum(kernel_ref[n] * spread, axis=0, keepdims=True)
            scaled = predicted * weight_ref[pl.ds(n, 1), :]
            scaled_ref[pl.ds(n, 1), :] = scaled
            return square + predicted * scaled

        return lax.fori_loop(0, rows, predict_step, zero[:1], unroll=8)

    def put_adjoint(step):
        def adjoint_step(n, acc):
            return acc + kernel_ref[n] * scaled_ref[pl.ds(n, 1), :]

        put_terms(step, lax.fori_loop(0, rows, adjoint_step, zero, unroll=4))

    def two_parts(field):
        high = field.astype(jnp.bfloat16)
        return high, (field - high.astype(jnp.float32)).astype(jnp.bfloat16)

    def parts_dot(map_ref, field):
        high, low = two_parts(field)
        parts = jnp.concatenate([high, low, high], axis=0)
        return one_hot_dot(map_ref[...], parts, (((1,), (0,)), ((), ())))

    def gram_dot(field):
        return parts_dot(gram_parts_ref, field)

    def row_of(a, b):
        return jnp.sum(a * b, axis=0, keepdims=True)

    residual_both = collected(0)
    spread_both = gram_dot(residual_both)
    residual, spread = residual_both[:, :LANES], spread_both[:, :LANES]
    spread_ref[...] = spread_both[:, LANES:]

    def predict(p, begin):
        def predict_step(n, carry):
            total = None if begin else predicted_ref[n]
            for _, chunk in chunks_of(p):
                part = pl.ds(chunk * SUB, SUB)
                product = kernel_ref[n, part, :] * spread_ref[part, :]
                total = product if total is None else total + product
            predicted_ref[n] = total
            return carry

        lax.fori_loop(0, rows, predict_step, 0, unroll=8)

    with scope("predict"):
        for p in range(early):
            predict(p, p == 0)
    with scope("takelast"):
        for p in range(early, piece_count):
            take(p)
            predict(p, False)

    def scale_step(n, carry):
        predicted = jnp.sum(predicted_ref[n], axis=0, keepdims=True)
        scaled_ref[pl.ds(n, 1), :] = predicted * weight_ref[pl.ds(n, 1), :]
        return carry

    with scope("adjoint1"):
        lax.fori_loop(0, rows, scale_step, 0, unroll=8)
        put_adjoint(1)
    with scope("collect1"):
        applied_both = residual_both + collected(1)

    def share_row(ref, send_sem, recv_sem, place, targets):
        copies = [
            pltpu.make_async_remote_copy(
                src_ref=ref.at[place], dst_ref=ref.at[place], send_sem=send_sem, recv_sem=recv_sem,
                device_id=target, device_id_type=MESH,
            )
            for target in targets
        ]
        for copy in copies:
            copy.start()

    def wait_rows(ref, send_sem, recv_sem, count):
        others = ref.at[pl.ds(0, count)]
        pltpu.make_async_copy(others, others, recv_sem).wait()
        pltpu.make_async_copy(others, others, send_sem).wait()

    group_targets = [coords(other(k)) for k in range(1, group)]
    control = direction = image = spread_image = image_applied = None
    norm_last = step_last = None
    for step in range(ITERS - 2):
        applied = applied_both[:, :LANES]
        parts_ref[step, me, 0:1] = row_of(residual, spread)
        parts_ref[step, me, 1:2] = row_of(applied, spread)
        with scope("sendsum"):
            share_row(parts_ref.at[step], sum_send.at[step], sum_recv.at[step], me, group_targets)
        with scope("normal"):
            next_spread = gram_dot(applied_both)
            put_normal(step + 2, next_spread[:, LANES:])
        with scope("waitsum"):
            wait_rows(parts_ref.at[step], sum_send.at[step], sum_recv.at[step], group - 1)
        total = jnp.sum(parts_ref[step], axis=0)
        total = jnp.sum(total, axis=1, keepdims=True)
        norm_now, curve = total[0:1], total[1:2]
        if step == 0:
            length = norm_now / curve
            direction, image = residual, applied
            control = length * direction
        else:
            ratio = norm_now / norm_last
            length = norm_now / (curve - ratio * norm_now / step_last)
            direction = residual + ratio * direction
            image = applied + ratio * image
            control = control + length * direction
        residual = residual - length * image
        if step == 0:
            spread_image = next_spread[:, :LANES]
            image_applied = applied_both + collected(step + 2)
        else:
            spread_image = next_spread[:, :LANES] + ratio * spread_image
            image_applied = applied_both + collected(step + 2) + ratio * image_applied
        spread = spread - length * spread_image
        applied_both = applied_both - length * image_applied
        norm_last, step_last = norm_now, length

    applied, image_applied = applied_both[:, :LANES], image_applied[:, :LANES]
    with scope("normal"):
        next_spread_both = gram_dot(applied_both)
        square = predict_all(next_spread_both[:, LANES:])
    next_spread = next_spread_both[:, :LANES]
    pairs = (
        (residual, spread), (applied, spread), (image, spread), (applied, next_spread),
        (image, next_spread), (image, spread_image), (image_applied, next_spread), (image_applied, spread_image),
    )
    wide = [row_of(a, b) * 0.5 for a, b in pairs] + [square]
    spot = lax.broadcasted_iota(jnp.int32, (1, LANES), 1)
    row = jnp.zeros((1, LANES), jnp.float32)
    for i, value in enumerate(wide):
        row = jnp.where(spot == i, jnp.sum(value, axis=1, keepdims=True), row)
    finals_ref[rank] = row
    with scope("sendsum"):
        share_row(finals_ref, final_send, final_recv, rank, [any_other(k) for k in range(1, device_count)])
    with scope("lastadjoint"):
        put_adjoint(ITERS)
    seen = gram_dot(jnp.concatenate([control, direction], axis=1))
    control_out, direction_out = seen[:, :LANES], seen[:, LANES:]
    felt = parts_dot(cov_parts_ref, jnp.concatenate([residual, applied, image, image_applied], axis=1))
    residual_felt, applied_felt, image_felt, twice_felt = [felt[:, i * LANES : (i + 1) * LANES] for i in range(4)]
    last_felt = applied_felt + parts_dot(cov_parts_ref, collected(ITERS)[:, :LANES])
    with scope("waitsum"):
        wait_rows(finals_ref, final_send, final_recv, device_count - 1)
    total = jnp.sum(finals_ref[...], axis=0)
    sums = [jnp.sum(jnp.where(spot == i, total, 0.0), axis=1, keepdims=True) for i in range(len(wide))]
    norm_now, curve, rest_image, next_next, image_next, image_image, twice_next, twice_image, square = sums
    ratio = norm_now / norm_last
    length = norm_now / (curve - ratio * norm_now / step_last)
    along = curve + ratio * rest_image
    image_square = next_next + ratio * (2.0 * image_next + ratio * image_image)
    norm_next = norm_now - length * (2.0 * along - length * image_square)
    cross = next_next + ratio * image_next
    image_curve = next_next + square + ratio * (2.0 * twice_next + ratio * twice_image)
    curve_next = curve - length * (2.0 * cross - length * image_curve)
    ratio_next = norm_next / norm_now
    length_next = norm_next / (curve_next - ratio_next * norm_next / length)
    direction_out = spread + ratio * direction_out
    spread_image = next_spread + ratio * spread_image
    control_out = control_out + length * direction_out
    control_out = control_out + length_next * (spread - length * spread_image + ratio_next * direction_out)
    image_felt = applied_felt + ratio * image_felt
    residual_felt = residual_felt - length * image_felt
    applied_felt = applied_felt - length * (last_felt + ratio * twice_felt)
    residual_felt = residual_felt - length_next * (applied_felt + ratio_next * image_felt)
    fields = (control_out, residual_felt)
    staged = [field[:LANES] for field in fields] + [field[LANES:] for field in fields]
    staged.append(jnp.zeros((LANES - 4 * SUB, LANES), jnp.float32))
    staged = jnp.concatenate(staged, axis=0).astype(jnp.bfloat16)
    straight = one_hot((LANES, LANES), lambda r: r)
    turned = one_hot_dot(straight, staged).astype(jnp.bfloat16)
    back_ref[0, 0:obs_count] = turned.reshape(obs_count, GRID_BLK, SUB, 3 * LANES)

    with scope("sendback"):
        for k in range(1, group):
            member = other(k)
            pltpu.make_async_remote_copy(
                src_ref=back_ref.at[0, top * half_obs + member // chan_count],
                dst_ref=back_ref.at[1, me],
                send_sem=back_send,
                recv_sem=back_recv,
                device_id=coords(member),
                device_id_type=MESH,
            ).start()
    back_ref[1, me] = back_ref[0, obs]
    for p in range(piece_count):
        others = put_ref.at[pl.ds(0, group - 1), span(p)]
        pltpu.make_async_copy(others, others, jac_send.at[p]).wait()
    others = back_ref.at[1, pl.ds(0, group - 1)]
    with scope("waitback"):
        pltpu.make_async_copy(others, others, back_recv).wait()
    pltpu.make_async_copy(others, others, back_send).wait()
    for block in range(GRID_BLK):
        spots = slice(block * BLOCK, (block + 1) * BLOCK)
        turned = [
            one_hot_dot(straight, back_ref[1, :, block, :, i * LANES : (i + 1) * LANES].reshape(group * SUB, LANES))
            for i in range(3)
        ]
        for which, out_ref in enumerate((increment_ref, residual_ref)):
            out_ref[0:LANES, spots] = turned[which].astype(jnp.bfloat16)
            first = which * 2 * SUB
            out_ref[LANES:layers, spots] = turned[2][first : first + layers - LANES].astype(jnp.bfloat16)


def half_slice_columns(jacobian, departures, obs_weights, column_count, grid_block, sqrt_cov):
    obs_count, chan_count = lax.axis_size("obs"), lax.axis_size("chan")
    group = obs_count // 2 * chan_count
    capacity, channels, layers = jacobian.shape
    mine = capacity // BLOCK * SUB
    padded = LANES + 2 * SUB
    chunk_count = padded // SUB
    piece_count = len(PIECES)
    rows = channels * chan_count // 2
    width = SUB * channels

    out = pltpu.VMEM((layers, GRID_BLK * BLOCK), jnp.bfloat16)
    hbm = pl.BlockSpec(memory_space=pltpu.HBM)
    vmem = pl.BlockSpec(memory_space=pltpu.VMEM)
    dma = pltpu.SemaphoreType.DMA
    bf16, f32 = jnp.bfloat16, jnp.float32
    increment, residual = pl.pallas_call(
        functools.partial(cg_kernel, obs_count, chan_count),
        out_shape=(out, out),
        in_specs=[hbm] * 6,
        out_specs=(vmem, vmem),
        scratch_shapes=[
            pltpu.VMEM(obs_weights.shape, f32),
            pltpu.VMEM(departures.shape, f32),
            pltpu.SMEM(column_count.shape, jnp.int32),
            pltpu.SMEM(grid_block.shape, jnp.int32),
            pltpu.VMEM(sqrt_cov.shape, f32),
            pltpu.VMEM((padded, channels, capacity), bf16),
            pltpu.VMEM((padded, capacity), f32),
            pltpu.VMEM((channels, capacity), f32),
            pltpu.VMEM((group, chunk_count, mine, width), bf16),
            pltpu.VMEM((group, chunk_count, mine, width), bf16),
            pltpu.VMEM((rows, padded, LANES), f32),
            pltpu.VMEM((rows, LANES), f32),
            pltpu.VMEM((capacity, capacity), bf16),
            pltpu.VMEM((width, width), bf16),
            pltpu.VMEM((padded, padded), f32),
            pltpu.VMEM((padded, 3 * padded), bf16),
            pltpu.VMEM((padded, padded), f32),
            pltpu.VMEM((padded, 3 * padded), bf16),
            pltpu.VMEM((padded, LANES), f32),
            pltpu.VMEM((rows, SUB, LANES), f32),
            pltpu.VMEM((rows, LANES), f32),
            pltpu.VMEM((2, 2 * LANES, 2 * LANES), bf16),
            pltpu.VMEM((2, SUB, LANES), f32),
            pltpu.VMEM((STEPS, 2, padded // 2, LANES), jnp.int16),
            pltpu.VMEM((STEPS, 2, 1, LANES), f32),
            pltpu.VMEM((ITERS - 2, group, 2, LANES), f32),
            pltpu.VMEM((obs_count * chan_count, 1, LANES), f32),
            pltpu.VMEM((2, group, GRID_BLK, SUB, 3 * LANES), bf16),
            dma((5,)), dma((LOADS,)),
            dma((piece_count,)), dma((piece_count,)),
            dma, dma,
            dma((STEPS, 2)), dma((STEPS, 2)),
            dma((ITERS - 2,)), dma((ITERS - 2,)),
            dma, dma,
            dma, dma,
        ],
        compiler_params=pltpu.CompilerParams(
            collective_id=0, has_side_effects=True, vmem_limit_bytes=VMEM_BYTES
        ),
    )(jacobian.transpose(2, 1, 0), obs_weights, departures, column_count, grid_block, sqrt_cov)
    return increment.T.astype(f32), residual.T.astype(f32)


def solution(mesh):
    obs_count, chan_count = mesh.shape["obs"], mesh.shape["chan"]
    group = obs_count // 2 * chan_count

    def plan(jacobian, departures, obs_weights, column_count, grid_block, sqrt_cov):
        capacity, channels, layers = jacobian.shape
        mine = capacity // BLOCK * SUB
        fits = (
            obs_count % 2 == 0
            and chan_count % 2 == 0
            and group * SUB == BLOCK
            and obs_count * mine == LANES
            and obs_count * GRID_BLK * SUB == LANES
            and chan_count == 4
            and channels == 32
            and LANES + SUB < layers <= LANES + 2 * SUB - 7
            and sum(PIECES) * SUB == LANES + 2 * SUB
        )
        chosen = half_slice_columns if fits else exchange_per_step
        return chosen(jacobian, departures, obs_weights, column_count, grid_block, sqrt_cov)

    in_specs = (P("obs", "chan", None), P("chan", "obs"), P("chan", "obs"), P("obs"), P("obs"), P())
    out_specs = (P("obs", None), P("obs", None))
    return jax.shard_map(plan, mesh=mesh, in_specs=in_specs, out_specs=out_specs, check_vma=False)
```

```python
import contextlib
import functools
import jax
import jax.numpy as jnp
from jax import lax
from jax.experimental import pallas as pl
from jax.experimental.pallas import tpu as pltpu
from jax.sharding import PartitionSpec as P

BLOCK = 128
ITERS = 5
GRID_BLK = 2
HIGHEST = lax.Precision.HIGHEST
MESH = pl.DeviceIdType.MESH


def block_terms(jac_part, weight_part, mask_part, predicted):
    scaled = (mask_part[:, None] * weight_part * predicted).astype(jnp.bfloat16)
    return lax.dot_general(
        jac_part, scaled, (((1,), (1,)), ((0,), (0,))), preferred_element_type=jnp.float32
    )


def forward_terms(jac_part, weight_part, mask_part, field_part):
    predicted = lax.dot_general(
        jac_part, field_part, (((2,), (1,)), ((0,), (0,))), preferred_element_type=jnp.float32
    )
    return block_terms(jac_part, weight_part, mask_part, predicted)


def exchange_per_step(jacobian, departures, obs_weights, column_count, grid_block, sqrt_cov):
    obs_count = lax.axis_size("obs")
    myself = lax.axis_index("obs")
    capacity, group_channels, layers = jacobian.shape
    block_count = capacity // BLOCK
    weight_cols = obs_weights.T
    depart_cols = departures.T
    observed = (jnp.arange(capacity, dtype=jnp.int32) < column_count[0]).astype(jnp.float32)
    every_id = lax.all_gather(grid_block, "obs", axis=0, tiled=True).reshape(obs_count, block_count)
    targets = jnp.arange(obs_count, dtype=jnp.int32)
    send_pick = (grid_block[None, :] // GRID_BLK == targets[:, None]).astype(jnp.float32)
    owned_here = every_id // GRID_BLK == myself
    places = every_id % GRID_BLK
    grid_index = jnp.arange(GRID_BLK, dtype=jnp.int32)
    take_pick = jnp.sum(
        ((places[None] == grid_index[:, None, None]) & owned_here[None]).astype(jnp.float32), axis=2
    )
    share_cols = BLOCK

    def local_terms(kernel_fn, inputs):
        return kernel_fn(jacobian, weight_cols, observed, inputs)

    def to_owners(terms):
        blocked = terms.reshape(block_count, BLOCK, layers)
        blocked = lax.psum(blocked, "chan")
        outgoing = jnp.dot(
            send_pick, blocked.reshape(block_count, -1), precision=lax.Precision.HIGHEST
        )
        incoming = lax.all_to_all(
            outgoing.reshape(obs_count, share_cols, layers),
            "obs",
            split_axis=0,
            concat_axis=0,
            tiled=True,
        )
        summed = jnp.dot(
            take_pick, incoming.reshape(obs_count, -1), precision=lax.Precision.HIGHEST
        )
        return summed.reshape(GRID_BLK, share_cols, layers)

    def spread(field):
        return jnp.dot(
            field.reshape(-1, layers), sqrt_cov, precision=lax.Precision.HIGHEST
        ).reshape(field.shape)

    def spread_back(field):
        flat = lax.dot_general(
            field.reshape(-1, layers),
            sqrt_cov,
            (((1,), (1,)), ((), ())),
            precision=lax.Precision.HIGHEST,
        )
        return flat.reshape(field.shape)

    def squared(values):
        partial_sum = jnp.sum(values * values)
        return lax.psum(partial_sum, "obs")

    residual = spread_back(to_owners(local_terms(block_terms, depart_cols)))
    control = jnp.zeros_like(residual)
    direction = residual
    norm_now = squared(residual)
    for iteration in range(ITERS):
        rounded = spread(direction).astype(jnp.bfloat16).reshape(GRID_BLK, -1)
        to_outgoing = jnp.dot(
            take_pick.T.astype(jnp.bfloat16), rounded, preferred_element_type=jnp.float32
        ).astype(jnp.bfloat16)
        to_incoming = lax.all_to_all(
            to_outgoing.reshape(obs_count, share_cols, layers),
            "obs",
            split_axis=0,
            concat_axis=0,
            tiled=True,
        )
        picked = jnp.dot(
            send_pick.T.astype(jnp.bfloat16),
            to_incoming.reshape(obs_count, -1),
            preferred_element_type=jnp.float32,
        )
        picked = picked.astype(jnp.bfloat16).reshape(block_count, share_cols, layers)
        fetched = picked.reshape(capacity, layers)
        image = direction + spread_back(to_owners(local_terms(forward_terms, fetched)))
        curvature_partial_sum = jnp.sum(direction * image)
        step_length = norm_now / lax.psum(curvature_partial_sum, "obs")
        control = control + step_length * direction
        residual = residual - step_length * image
        norm_next = squared(residual)
        direction = residual + norm_next / norm_now * direction
        norm_now = norm_next
    increment = spread(control)
    return (increment.reshape(-1, layers), residual.reshape(-1, layers))


LANES = 128
SUB = 8
LEVELS = 32000.0
PIECES = (1, 3, 3, 4, 4, 2, 1)
AHEAD = 3
LATE = 2
LOADS = 4
VMEM_BYTES = 67043328 - 1024 * 1024
STEPS = ITERS + 1
scope = lambda name: contextlib.nullcontext()
NT = (((1,), (1,)), ((), ()))
TN = (((0,), (0,)), ((), ()))


def exact_dot(a, b, dims):
    return lax.dot_general(a, b, dims, precision=HIGHEST, preferred_element_type=jnp.float32)


def one_hot_dot(a, b, dims=NT):
    return lax.dot_general(a, b, dims, preferred_element_type=jnp.float32)


def far_first(count):
    return sorted(range(1, count), key=lambda k: -bin(k // 2).count("1"))


def cg_kernel(
    obs_count, chan_count, jac_ref, *rest
):
    smalls, (increment_ref, residual_ref), rest = rest[:5], rest[5:7], rest[7:]
    run_cg(obs_count, chan_count, jac_ref, smalls, rest[:5], increment_ref, residual_ref, *rest[5:])


def run_cg(
    obs_count, chan_count, jac_ref, small_hbm, small_refs, increment_ref, residual_ref,
    jac_vmem, source_ref, mixed_ref, put_ref, got_ref, kernel_ref, weight_ref, order_ref, back_order_ref,
    gram_ref, gram_parts_ref, cov_pad_ref, cov_parts_ref, spread_ref, predicted_ref, scaled_ref, relation_ref, id_ref, terms_ref, scale_ref, parts_ref, finals_ref, back_ref,
    small_sem, load_sem, jac_send, jac_recv, id_send, id_recv, term_send, term_recv, sum_send, sum_recv,
    final_send, final_recv, back_send, back_recv
):
    obs_weight_ref, depart_ref, count_ref, block_ref, cov_ref = small_refs
    small_loads = [
        pltpu.make_async_copy(source, target, small_sem.at[i])
        for i, (source, target) in enumerate(zip(small_hbm, small_refs))
    ]
    for copy in small_loads:
        copy.start()
    layers, channels, columns = jac_ref.shape
    padded = jac_vmem.shape[0]
    bounds = [layers // SUB * (i + 1) // LOADS * SUB for i in range(LOADS - 1)]
    bounds = list(zip([0] + bounds, bounds + [layers]))
    loads = [
        pltpu.make_async_copy(jac_ref.at[pl.ds(a, b - a)], jac_vmem.at[pl.ds(a, b - a)], load_sem.at[i])
        for i, (a, b) in enumerate(bounds)
    ]
    for copy in loads:
        copy.start()
    chunk_count = padded // SUB
    piece_count = len(PIECES)
    half_obs = obs_count // 2
    group = half_obs * chan_count
    rows = kernel_ref.shape[0]
    lows = chan_count // 2
    block_count = columns // BLOCK
    mine = block_count * SUB

    obs, chan = lax.axis_index("obs"), lax.axis_index("chan")
    top = obs // half_obs
    me = (obs % half_obs) * chan_count + chan
    slot = (chan % lows) * (2 * half_obs) + (chan // lows) * half_obs + obs % half_obs

    def coords(member):
        return (top * half_obs + member // chan_count, member % chan_count)

    def other(k):
        member, place = 0, 1
        while place < group:
            member = member + (me // place + k // place) % 2 * place
            place *= 2
        return member

    device_count = obs_count * chan_count
    rank = obs * chan_count + chan

    def any_other(k):
        member, place = 0, 1
        while place < device_count:
            member = member + (rank // place + k // place) % 2 * place
            place *= 2
        return (member // chan_count, member % chan_count)

    partner = ((obs + half_obs) % obs_count, chan)
    barrier = pltpu.get_barrier_semaphore()

    def greet(k):
        pl.semaphore_signal(barrier, inc=1, device_id=coords(other(k)), device_id_type=MESH)

    for k in far_first(group):
        greet(k)
    pl.semaphore_signal(barrier, inc=1, device_id=partner, device_id_type=MESH)

    chunks = [chunk_count - 1] + list(range(chunk_count - 1))
    starts = [sum(PIECES[:p]) for p in range(piece_count)]
    def one_hot(shape, wanted):
        row = lax.broadcasted_iota(jnp.int32, shape, 0)
        column = lax.broadcasted_iota(jnp.int32, shape, 1)
        return jnp.where(column == wanted(row), 1.0, 0.0).astype(jnp.bfloat16)

    order_ref[...] = one_hot(
        (columns, columns), lambda r: r % mine // SUB * BLOCK + r // mine * SUB + r % SUB
    )
    width = SUB * channels
    back_order_ref[...] = one_hot((width, width), lambda r: r % SUB * channels + r // SUB)

    with scope("smallwait"):
        for copy in small_loads:
            copy.wait()
    place = lax.broadcasted_iota(jnp.int32, (channels, columns), 1)
    weight = jnp.where(place < count_ref[0], obs_weight_ref[...], 0.0)
    weight_high = weight.astype(jnp.bfloat16)
    jac_vmem[layers] = weight_high
    jac_vmem[layers + 1] = (weight - weight_high.astype(jnp.float32)).astype(jnp.bfloat16)
    scaled = (weight * depart_ref[...]).astype(jnp.bfloat16).astype(jnp.float32)

    def source_rows(first, count):
        block = jac_vmem[pl.ds(first, count)].astype(jnp.float32)
        source_ref[pl.ds(first, count)] = jnp.sum(block * scaled[None], axis=1)

    def source_step(q, carry):
        source_rows(q * SUB, SUB)
        return carry

    for copy, (a, b) in zip(loads, bounds):
        with scope("loadwait"):
            copy.wait()
        with scope("source"):
            lax.fori_loop(a // SUB, b // SUB, source_step, 0)
    source_rows(layers // SUB * SUB, layers % SUB)
    mixed_ref[...] = jnp.zeros((channels, columns), jnp.float32)
    for k in range(block_count):
        mixed_ref[0:1, k * BLOCK : (k + 1) * BLOCK] = jnp.full((1, BLOCK), block_ref[k].astype(jnp.float32))
    mixed_ref[1 : 1 + layers - LANES] = source_ref[LANES:layers]
    jac_vmem[layers + 2] = mixed_ref[...].astype(jnp.bfloat16)
    source_slots = LANES // channels
    for q in range(source_slots):
        jac_vmem[layers + 3 + q] = source_ref[q * channels : (q + 1) * channels].astype(jnp.bfloat16)
    for extra in range(layers + 3 + source_slots, padded):
        jac_vmem[extra] = jnp.zeros((channels, columns), jnp.bfloat16)

    def span(p):
        return pl.ds(starts[p], PIECES[p])

    def chunks_of(p):
        return [(i, chunks[i]) for i in range(starts[p], starts[p] + PIECES[p])]

    def stage(p):
        for i, chunk in chunks_of(p):
            block = jac_vmem[chunk * SUB : (chunk + 1) * SUB].reshape(width, columns)
            turned = one_hot_dot(order_ref[...], block).astype(jnp.bfloat16)
            put_ref[:, i] = turned.reshape(group, mine, width)

    def send(p):
        def one(k, carry):
            member = other(k)
            pltpu.make_async_remote_copy(
                src_ref=put_ref.at[member, span(p)],
                dst_ref=got_ref.at[slot, span(p)],
                send_sem=jac_send.at[p],
                recv_sem=jac_recv.at[p],
                device_id=coords(member),
                device_id_type=MESH,
            ).start()
            return carry

        lax.fori_loop(1, group, one, 0)
        for i, _ in chunks_of(p):
            got_ref[slot, i] = put_ref[me, i]

    with scope("stage0"):
        stage(0)
    with scope("barrier"):
        pl.semaphore_wait(barrier, group)
    with scope("sends"):
        for p in range(AHEAD):
            if p:
                stage(p)
            send(p)
        for p in range(AHEAD, piece_count):
            stage(p)

    cov = cov_ref[...]
    gram_ref[...] = jnp.zeros(gram_ref.shape, jnp.float32)
    cov_pad_ref[...] = jnp.zeros(cov_pad_ref.shape, jnp.float32)
    gram = exact_dot(cov, cov, TN)
    gram_ref[0:layers, 0:layers] = gram
    gram_high = gram_ref[...].astype(jnp.bfloat16)
    gram_low = (gram_ref[...] - gram_high.astype(jnp.float32)).astype(jnp.bfloat16)
    gram_parts_ref[...] = jnp.concatenate([gram_high, gram_high, gram_low], axis=1)
    cov_pad_ref[0:layers, 0:layers] = cov
    cov_high = cov_pad_ref[...].astype(jnp.bfloat16)
    cov_low = (cov_pad_ref[...] - cov_high.astype(jnp.float32)).astype(jnp.bfloat16)
    cov_parts_ref[...] = jnp.concatenate([cov_high, cov_high, cov_low], axis=1)

    def take(p):
        others = got_ref.at[pl.ds(0, group - 1), span(p)]
        pltpu.make_async_copy(others, others, jac_recv.at[p]).wait()
        for i, chunk in chunks_of(p):
            block = got_ref[:, i].reshape(group * mine, width)
            turned = one_hot_dot(back_order_ref[...], block)
            for low in range(lows):
                part = turned[:, low * LANES : (low + 1) * LANES].reshape(channels, SUB, LANES)
                kernel_ref[low * channels : (low + 1) * channels, chunk * SUB : (chunk + 1) * SUB, :] = part

    half_rows = padded // 2
    lane = lax.broadcasted_iota(jnp.int32, (half_rows, LANES), 1)
    row_spot = lax.broadcasted_iota(jnp.int32, (half_rows, LANES), 0)

    def terms_copies(step):
        return [
            pltpu.make_async_remote_copy(
                src_ref=ref.at[step, 0], dst_ref=ref.at[step, 1],
                send_sem=term_send.at[step, i], recv_sem=term_recv.at[step, i],
                device_id=partner, device_id_type=MESH,
            )
            for i, ref in enumerate((scale_ref, terms_ref))
        ]

    def put_terms(step, terms):
        summed = terms + pltpu.roll(terms, LANES // 2, 1)
        lower = jnp.where(row_spot < layers - half_rows, summed[half_rows:], 0.0)
        packed = jnp.where(lane < LANES // 2, summed[:half_rows], lower)
        largest = jnp.maximum(jnp.max(jnp.abs(packed), axis=0, keepdims=True), 1e-30)
        scale_ref[step, 0] = largest * (1.0 / LEVELS)
        terms_ref[step, 0] = jnp.round(packed * (LEVELS / largest)).astype(jnp.int32).astype(jnp.int16)
        for copy in terms_copies(step):
            copy.start()

    with scope("take0"):
        take(0)
    weight_ref[...] = kernel_ref[:, layers, :] + kernel_ref[:, layers + 1, :]
    id_ref[0] = jnp.broadcast_to(kernel_ref[0, layers + 2 : layers + 3, :], (SUB, LANES))
    id_copy = pltpu.make_async_remote_copy(
        src_ref=id_ref.at[0], dst_ref=id_ref.at[1], send_sem=id_send, recv_sem=id_recv,
        device_id=partner, device_id_type=MESH,
    )
    id_copy.start()

    def low_sum(first, count, layer):
        return sum(
            kernel_ref[low * channels + first : low * channels + first + count, layer, :] for low in range(lows)
        )

    for q in range(source_slots):
        spread_ref[q * channels : (q + 1) * channels] = low_sum(0, channels, layers + 3 + q)
    spread_ref[LANES:padded] = jnp.zeros((padded - LANES, LANES), jnp.float32)
    spread_ref[LANES:layers] = low_sum(1, layers - LANES, layers + 2)
    put_terms(0, spread_ref[...])
    with scope("sends2"):
        for p in range(AHEAD, piece_count):
            send(p)
    early = piece_count - LATE
    with scope("takes"):
        for p in range(1, early):
            take(p)

    with scope("idwait"):
        id_copy.wait()
    grid_row = lax.broadcasted_iota(jnp.int32, (LANES, LANES), 0)
    grid_lane = lax.broadcasted_iota(jnp.int32, (LANES, LANES), 1)

    def pick_of(which):
        wanted = id_ref[which, 0:1, :].astype(jnp.int32) * SUB + grid_lane % SUB
        return jnp.where(grid_row == wanted, 1.0, 0.0).astype(jnp.bfloat16)

    own_pick = pick_of(0)
    both_picks = jnp.concatenate([own_pick, pick_of(1)], axis=1)
    matched = one_hot_dot(own_pick, both_picks, TN).astype(jnp.bfloat16)
    relation = jnp.concatenate([both_picks, matched], axis=0).astype(jnp.float32)
    relation_lane = lax.broadcasted_iota(jnp.int32, relation.shape, 1) % LANES
    for which in range(2):
        kept = relation_lane // (LANES // 2) == which
        relation_ref[which] = jnp.where(kept, relation, 0.0).astype(jnp.bfloat16)

    zero = jnp.zeros((padded, LANES), jnp.float32)

    def collected(step):
        with scope("waitterms"):
            for copy in terms_copies(step):
                copy.wait()
        both = [terms_ref[step, i].astype(jnp.int32).astype(jnp.float32) * scale_ref[step, i] for i in range(2)]
        both = jnp.concatenate(both, axis=1)
        high = both.astype(jnp.bfloat16)
        low = (both - high.astype(jnp.float32)).astype(jnp.bfloat16)
        parts = jnp.concatenate([high.astype(jnp.float32), low.astype(jnp.float32)], axis=0).astype(jnp.bfloat16)
        sums = [one_hot_dot(parts, relation_ref[which]) for which in range(2)]
        return jnp.concatenate([value[:half_rows] + value[half_rows:] for value in sums], axis=0)

    def put_normal(step, spread):
        def normal_step(n, acc):
            kernel = kernel_ref[n]
            predicted = jnp.sum(kernel * spread, axis=0, keepdims=True)
            return acc + kernel * (predicted * weight_ref[pl.ds(n, 1), :])

        put_terms(step, lax.fori_loop(0, rows, normal_step, zero, unroll=8))

    def predict_all(spread):
        def predict_step(n, square):
            predicted = jnp.sum(kernel_ref[n] * spread, axis=0, keepdims=True)
            scaled = predicted * weight_ref[pl.ds(n, 1), :]
            scaled_ref[pl.ds(n, 1), :] = scaled
            return square + predicted * scaled

        return lax.fori_loop(0, rows, predict_step, zero[:1], unroll=8)

    def put_adjoint(step):
        def adjoint_step(n, acc):
            return acc + kernel_ref[n] * scaled_ref[pl.ds(n, 1), :]

        put_terms(step, lax.fori_loop(0, rows, adjoint_step, zero, unroll=8))

    def two_parts(field):
        high = field.astype(jnp.bfloat16)
        return high, (field - high.astype(jnp.float32)).astype(jnp.bfloat16)

    def parts_dot(map_ref, field):
        high, low = two_parts(field)
        parts = jnp.concatenate([high, low, high], axis=0)
        return one_hot_dot(map_ref[...], parts, (((1,), (0,)), ((), ())))

    def gram_dot(field):
        return parts_dot(gram_parts_ref, field)

    def row_of(a, b):
        return jnp.sum(a * b, axis=0, keepdims=True)

    residual_both = collected(0)
    spread_both = gram_dot(residual_both)
    residual, spread = residual_both[:, :LANES], spread_both[:, :LANES]
    spread_ref[...] = spread_both[:, LANES:]

    def predict(p, begin):
        def predict_step(n, carry):
            total = None if begin else predicted_ref[n]
            for _, chunk in chunks_of(p):
                part = pl.ds(chunk * SUB, SUB)
                product = kernel_ref[n, part, :] * spread_ref[part, :]
                total = product if total is None else total + product
            predicted_ref[n] = total
            return carry

        lax.fori_loop(0, rows, predict_step, 0, unroll=8)

    with scope("predict"):
        for p in range(early):
            predict(p, p == 0)
    with scope("takelast"):
        for p in range(early, piece_count):
            take(p)
            predict(p, False)

    def scale_step(n, carry):
        predicted = jnp.sum(predicted_ref[n], axis=0, keepdims=True)
        scaled_ref[pl.ds(n, 1), :] = predicted * weight_ref[pl.ds(n, 1), :]
        return carry

    with scope("adjoint1"):
        lax.fori_loop(0, rows, scale_step, 0, unroll=8)
        put_adjoint(1)
    with scope("collect1"):
        applied_both = residual_both + collected(1)

    def share_row(ref, send_sem, recv_sem, place, targets):
        copies = [
            pltpu.make_async_remote_copy(
                src_ref=ref.at[place], dst_ref=ref.at[place], send_sem=send_sem, recv_sem=recv_sem,
                device_id=target, device_id_type=MESH,
            )
            for target in targets
        ]
        for copy in copies:
            copy.start()

    def wait_rows(ref, send_sem, recv_sem, count):
        others = ref.at[pl.ds(0, count)]
        pltpu.make_async_copy(others, others, recv_sem).wait()
        pltpu.make_async_copy(others, others, send_sem).wait()

    group_targets = [coords(other(k)) for k in far_first(group)]
    control = direction = image = spread_image = image_applied = None
    norm_last = step_last = None
    for step in range(ITERS - 2):
        applied = applied_both[:, :LANES]
        parts_ref[step, me, 0:1] = row_of(residual, spread)
        parts_ref[step, me, 1:2] = row_of(applied, spread)
        with scope("sendsum"):
            share_row(parts_ref.at[step], sum_send.at[step], sum_recv.at[step], me, group_targets)
        with scope("normal"):
            next_spread = gram_dot(applied_both)
            put_normal(step + 2, next_spread[:, LANES:])
        with scope("waitsum"):
            wait_rows(parts_ref.at[step], sum_send.at[step], sum_recv.at[step], group - 1)
        total = jnp.sum(parts_ref[step], axis=0)
        total = jnp.sum(total, axis=1, keepdims=True)
        norm_now, curve = total[0:1], total[1:2]
        if step == 0:
            length = norm_now / curve
            direction, image = residual, applied
            control = length * direction
        else:
            ratio = norm_now / norm_last
            length = norm_now / (curve - ratio * norm_now / step_last)
            direction = residual + ratio * direction
            image = applied + ratio * image
            control = control + length * direction
        residual = residual - length * image
        if step == 0:
            spread_image = next_spread[:, :LANES]
            image_applied = applied_both + collected(step + 2)
        else:
            spread_image = next_spread[:, :LANES] + ratio * spread_image
            image_applied = applied_both + collected(step + 2) + ratio * image_applied
        spread = spread - length * spread_image
        applied_both = applied_both - length * image_applied
        norm_last, step_last = norm_now, length

    applied, image_applied = applied_both[:, :LANES], image_applied[:, :LANES]
    with scope("normal"):
        next_spread_both = gram_dot(applied_both)
        square = predict_all(next_spread_both[:, LANES:])
    next_spread = next_spread_both[:, :LANES]
    pairs = (
        (residual, spread), (applied, spread), (image, spread), (applied, next_spread),
        (image, next_spread), (image, spread_image), (image_applied, next_spread), (image_applied, spread_image),
    )
    wide = [row_of(a, b) * 0.5 for a, b in pairs] + [square]
    spot = lax.broadcasted_iota(jnp.int32, (1, LANES), 1)
    row = jnp.zeros((1, LANES), jnp.float32)
    for i, value in enumerate(wide):
        row = jnp.where(spot == i, jnp.sum(value, axis=1, keepdims=True), row)
    finals_ref[rank] = row
    with scope("sendsum"):
        share_row(finals_ref, final_send, final_recv, rank, [any_other(k) for k in far_first(device_count)])
    with scope("lastadjoint"):
        put_adjoint(ITERS)
    seen = gram_dot(jnp.concatenate([control, direction], axis=1))
    control_out, direction_out = seen[:, :LANES], seen[:, LANES:]
    felt = parts_dot(cov_parts_ref, jnp.concatenate([residual, applied, image, image_applied], axis=1))
    residual_felt, applied_felt, image_felt, twice_felt = [felt[:, i * LANES : (i + 1) * LANES] for i in range(4)]
    last_felt = applied_felt + parts_dot(cov_parts_ref, collected(ITERS)[:, :LANES])
    with scope("waitsum"):
        wait_rows(finals_ref, final_send, final_recv, device_count - 1)
    total = jnp.sum(finals_ref[...], axis=0)
    sums = [jnp.sum(jnp.where(spot == i, total, 0.0), axis=1, keepdims=True) for i in range(len(wide))]
    norm_now, curve, rest_image, next_next, image_next, image_image, twice_next, twice_image, square = sums
    ratio = norm_now / norm_last
    length = norm_now / (curve - ratio * norm_now / step_last)
    along = curve + ratio * rest_image
    image_square = next_next + ratio * (2.0 * image_next + ratio * image_image)
    norm_next = norm_now - length * (2.0 * along - length * image_square)
    cross = next_next + ratio * image_next
    image_curve = next_next + square + ratio * (2.0 * twice_next + ratio * twice_image)
    curve_next = curve - length * (2.0 * cross - length * image_curve)
    ratio_next = norm_next / norm_now
    length_next = norm_next / (curve_next - ratio_next * norm_next / length)
    direction_out = spread + ratio * direction_out
    spread_image = next_spread + ratio * spread_image
    control_out = control_out + length * direction_out
    control_out = control_out + length_next * (spread - length * spread_image + ratio_next * direction_out)
    image_felt = applied_felt + ratio * image_felt
    residual_felt = residual_felt - length * image_felt
    applied_felt = applied_felt - length * (last_felt + ratio * twice_felt)
    residual_felt = residual_felt - length_next * (applied_felt + ratio_next * image_felt)
    fields = (control_out, residual_felt)
    staged = [field[:LANES] for field in fields] + [field[LANES:] for field in fields]
    staged.append(jnp.zeros((LANES - 4 * SUB, LANES), jnp.float32))
    staged = jnp.concatenate(staged, axis=0).astype(jnp.bfloat16)
    straight = one_hot((LANES, LANES), lambda r: r)
    turned = one_hot_dot(straight, staged).astype(jnp.bfloat16)
    back_ref[0, 0:obs_count] = turned.reshape(obs_count, GRID_BLK, SUB, 3 * LANES)

    with scope("sendback"):
        for k in far_first(group):
            member = other(k)
            pltpu.make_async_remote_copy(
                src_ref=back_ref.at[0, top * half_obs + member // chan_count],
                dst_ref=back_ref.at[1, me],
                send_sem=back_send,
                recv_sem=back_recv,
                device_id=coords(member),
                device_id_type=MESH,
            ).start()
    back_ref[1, me] = back_ref[0, obs]
    for p in range(piece_count):
        others = put_ref.at[pl.ds(0, group - 1), span(p)]
        pltpu.make_async_copy(others, others, jac_send.at[p]).wait()
    others = back_ref.at[1, pl.ds(0, group - 1)]
    with scope("waitback"):
        pltpu.make_async_copy(others, others, back_recv).wait()
    pltpu.make_async_copy(others, others, back_send).wait()
    for block in range(GRID_BLK):
        spots = slice(block * BLOCK, (block + 1) * BLOCK)
        turned = [
            one_hot_dot(straight, back_ref[1, :, block, :, i * LANES : (i + 1) * LANES].reshape(group * SUB, LANES))
            for i in range(3)
        ]
        for which, out_ref in enumerate((increment_ref, residual_ref)):
            out_ref[0:LANES, spots] = turned[which].astype(jnp.bfloat16)
            first = which * 2 * SUB
            out_ref[LANES:layers, spots] = turned[2][first : first + layers - LANES].astype(jnp.bfloat16)


def half_slice_columns(jacobian, departures, obs_weights, column_count, grid_block, sqrt_cov):
    obs_count, chan_count = lax.axis_size("obs"), lax.axis_size("chan")
    group = obs_count // 2 * chan_count
    capacity, channels, layers = jacobian.shape
    mine = capacity // BLOCK * SUB
    padded = LANES + 2 * SUB
    chunk_count = padded // SUB
    piece_count = len(PIECES)
    rows = channels * chan_count // 2
    width = SUB * channels

    out = pltpu.VMEM((layers, GRID_BLK * BLOCK), jnp.bfloat16)
    hbm = pl.BlockSpec(memory_space=pltpu.HBM)
    vmem = pl.BlockSpec(memory_space=pltpu.VMEM)
    dma = pltpu.SemaphoreType.DMA
    bf16, f32 = jnp.bfloat16, jnp.float32
    increment, residual = pl.pallas_call(
        functools.partial(cg_kernel, obs_count, chan_count),
        out_shape=(out, out),
        in_specs=[hbm] * 6,
        out_specs=(vmem, vmem),
        scratch_shapes=[
            pltpu.VMEM(obs_weights.shape, f32),
            pltpu.VMEM(departures.shape, f32),
            pltpu.SMEM(column_count.shape, jnp.int32),
            pltpu.SMEM(grid_block.shape, jnp.int32),
            pltpu.VMEM(sqrt_cov.shape, f32),
            pltpu.VMEM((padded, channels, capacity), bf16),
            pltpu.VMEM((padded, capacity), f32),
            pltpu.VMEM((channels, capacity), f32),
            pltpu.VMEM((group, chunk_count, mine, width), bf16),
            pltpu.VMEM((group, chunk_count, mine, width), bf16),
            pltpu.VMEM((rows, padded, LANES), f32),
            pltpu.VMEM((rows, LANES), f32),
            pltpu.VMEM((capacity, capacity), bf16),
            pltpu.VMEM((width, width), bf16),
            pltpu.VMEM((padded, padded), f32),
            pltpu.VMEM((padded, 3 * padded), bf16),
            pltpu.VMEM((padded, padded), f32),
            pltpu.VMEM((padded, 3 * padded), bf16),
            pltpu.VMEM((padded, LANES), f32),
            pltpu.VMEM((rows, SUB, LANES), f32),
            pltpu.VMEM((rows, LANES), f32),
            pltpu.VMEM((2, 2 * LANES, 2 * LANES), bf16),
            pltpu.VMEM((2, SUB, LANES), f32),
            pltpu.VMEM((STEPS, 2, padded // 2, LANES), jnp.int16),
            pltpu.VMEM((STEPS, 2, 1, LANES), f32),
            pltpu.VMEM((ITERS - 2, group, 2, LANES), f32),
            pltpu.VMEM((obs_count * chan_count, 1, LANES), f32),
            pltpu.VMEM((2, group, GRID_BLK, SUB, 3 * LANES), bf16),
            dma((5,)), dma((LOADS,)),
            dma((piece_count,)), dma((piece_count,)),
            dma, dma,
            dma((STEPS, 2)), dma((STEPS, 2)),
            dma((ITERS - 2,)), dma((ITERS - 2,)),
            dma, dma,
            dma, dma,
        ],
        compiler_params=pltpu.CompilerParams(
            collective_id=0, has_side_effects=True, vmem_limit_bytes=VMEM_BYTES
        ),
    )(jacobian.transpose(2, 1, 0), obs_weights, departures, column_count, grid_block, sqrt_cov)
    return increment.T.astype(f32), residual.T.astype(f32)


def solution(mesh):
    obs_count, chan_count = mesh.shape["obs"], mesh.shape["chan"]
    group = obs_count // 2 * chan_count

    def plan(jacobian, departures, obs_weights, column_count, grid_block, sqrt_cov):
        capacity, channels, layers = jacobian.shape
        mine = capacity // BLOCK * SUB
        fits = (
            obs_count % 2 == 0
            and chan_count % 2 == 0
            and group * SUB == BLOCK
            and obs_count * mine == LANES
            and obs_count * GRID_BLK * SUB == LANES
            and chan_count == 4
            and channels == 32
            and LANES + SUB < layers <= LANES + 2 * SUB - 7
            and sum(PIECES) * SUB == LANES + 2 * SUB
        )
        chosen = half_slice_columns if fits else exchange_per_step
        return chosen(jacobian, departures, obs_weights, column_count, grid_block, sqrt_cov)

    in_specs = (P("obs", "chan", None), P("chan", "obs"), P("chan", "obs"), P("obs"), P("obs"), P())
    out_specs = (P("obs", None), P("obs", None))
    return jax.shard_map(plan, mesh=mesh, in_specs=in_specs, out_specs=out_specs, check_vma=False)
```

```python
import functools
import jax
import jax.numpy as jnp
from jax import lax
from jax.experimental import pallas as pl
from jax.experimental.pallas import tpu as pltpu
from jax.sharding import PartitionSpec as P

BLOCK = 128
ITERS = 5
GRID_BLK = 2
HIGHEST = lax.Precision.HIGHEST
MESH = pl.DeviceIdType.MESH


def block_terms(jac_part, weight_part, mask_part, predicted):
    scaled = (mask_part[:, None] * weight_part * predicted).astype(jnp.bfloat16)
    return lax.dot_general(
        jac_part, scaled, (((1,), (1,)), ((0,), (0,))), preferred_element_type=jnp.float32
    )


def forward_terms(jac_part, weight_part, mask_part, field_part):
    predicted = lax.dot_general(
        jac_part, field_part, (((2,), (1,)), ((0,), (0,))), preferred_element_type=jnp.float32
    )
    return block_terms(jac_part, weight_part, mask_part, predicted)


def exchange_per_step(jacobian, departures, obs_weights, column_count, grid_block, sqrt_cov):
    obs_count = lax.axis_size("obs")
    myself = lax.axis_index("obs")
    capacity, group_channels, layers = jacobian.shape
    block_count = capacity // BLOCK
    weight_cols = obs_weights.T
    depart_cols = departures.T
    observed = (jnp.arange(capacity, dtype=jnp.int32) < column_count[0]).astype(jnp.float32)
    every_id = lax.all_gather(grid_block, "obs", axis=0, tiled=True).reshape(obs_count, block_count)
    targets = jnp.arange(obs_count, dtype=jnp.int32)
    send_pick = (grid_block[None, :] // GRID_BLK == targets[:, None]).astype(jnp.float32)
    owned_here = every_id // GRID_BLK == myself
    places = every_id % GRID_BLK
    grid_index = jnp.arange(GRID_BLK, dtype=jnp.int32)
    take_pick = jnp.sum(
        ((places[None] == grid_index[:, None, None]) & owned_here[None]).astype(jnp.float32), axis=2
    )
    share_cols = BLOCK

    def local_terms(kernel_fn, inputs):
        return kernel_fn(jacobian, weight_cols, observed, inputs)

    def to_owners(terms):
        blocked = terms.reshape(block_count, BLOCK, layers)
        blocked = lax.psum(blocked, "chan")
        outgoing = jnp.dot(
            send_pick, blocked.reshape(block_count, -1), precision=lax.Precision.HIGHEST
        )
        incoming = lax.all_to_all(
            outgoing.reshape(obs_count, share_cols, layers),
            "obs",
            split_axis=0,
            concat_axis=0,
            tiled=True,
        )
        summed = jnp.dot(
            take_pick, incoming.reshape(obs_count, -1), precision=lax.Precision.HIGHEST
        )
        return summed.reshape(GRID_BLK, share_cols, layers)

    def spread(field):
        return jnp.dot(
            field.reshape(-1, layers), sqrt_cov, precision=lax.Precision.HIGHEST
        ).reshape(field.shape)

    def spread_back(field):
        flat = lax.dot_general(
            field.reshape(-1, layers),
            sqrt_cov,
            (((1,), (1,)), ((), ())),
            precision=lax.Precision.HIGHEST,
        )
        return flat.reshape(field.shape)

    def squared(values):
        partial_sum = jnp.sum(values * values)
        return lax.psum(partial_sum, "obs")

    residual = spread_back(to_owners(local_terms(block_terms, depart_cols)))
    control = jnp.zeros_like(residual)
    direction = residual
    norm_now = squared(residual)
    for iteration in range(ITERS):
        rounded = spread(direction).astype(jnp.bfloat16).reshape(GRID_BLK, -1)
        to_outgoing = jnp.dot(
            take_pick.T.astype(jnp.bfloat16), rounded, preferred_element_type=jnp.float32
        ).astype(jnp.bfloat16)
        to_incoming = lax.all_to_all(
            to_outgoing.reshape(obs_count, share_cols, layers),
            "obs",
            split_axis=0,
            concat_axis=0,
            tiled=True,
        )
        picked = jnp.dot(
            send_pick.T.astype(jnp.bfloat16),
            to_incoming.reshape(obs_count, -1),
            preferred_element_type=jnp.float32,
        )
        picked = picked.astype(jnp.bfloat16).reshape(block_count, share_cols, layers)
        fetched = picked.reshape(capacity, layers)
        image = direction + spread_back(to_owners(local_terms(forward_terms, fetched)))
        curvature_partial_sum = jnp.sum(direction * image)
        step_length = norm_now / lax.psum(curvature_partial_sum, "obs")
        control = control + step_length * direction
        residual = residual - step_length * image
        norm_next = squared(residual)
        direction = residual + norm_next / norm_now * direction
        norm_now = norm_next
    increment = spread(control)
    return (increment.reshape(-1, layers), residual.reshape(-1, layers))


LANES = 128
SUB = 8
LEVELS = 32000.0
PIECES = (2,) * 9
AHEAD = 3
LATE = 2
LOADS = 4
VMEM_BYTES = 67043328 - 1024 * 1024
STEPS = ITERS + 1
NT = (((1,), (1,)), ((), ()))
TN = (((0,), (0,)), ((), ()))


def exact_dot(a, b, dims):
    return lax.dot_general(a, b, dims, precision=HIGHEST, preferred_element_type=jnp.float32)


def one_hot_dot(a, b, dims=NT):
    return lax.dot_general(a, b, dims, preferred_element_type=jnp.float32)


def far_first(count):
    return sorted(range(1, count), key=lambda k: -bin(k // 2).count("1"))


def cg_kernel(
    obs_count, chan_count, jac_ref, *rest
):
    smalls, (increment_ref, residual_ref), rest = rest[:5], rest[5:7], rest[7:]
    run_cg(obs_count, chan_count, jac_ref, smalls, rest[:5], increment_ref, residual_ref, *rest[5:])


def run_cg(
    obs_count, chan_count, jac_ref, small_hbm, small_refs, increment_ref, residual_ref,
    jac_vmem, source_ref, mixed_ref, put_ref, got_ref, kernel_ref, weight_ref, order_ref, back_order_ref,
    gram_ref, gram_parts_ref, cov_pad_ref, cov_parts_ref, spread_ref, predicted_ref, scaled_ref, relation_ref, id_ref, terms_ref, scale_ref, parts_ref, finals_ref, back_ref,
    small_sem, load_sem, jac_send, jac_recv, id_send, id_recv, term_send, term_recv, sum_send, sum_recv,
    final_send, final_recv, back_send, back_recv
):
    obs_weight_ref, depart_ref, count_ref, block_ref, cov_ref = small_refs
    small_loads = [
        pltpu.make_async_copy(source, target, small_sem.at[i])
        for i, (source, target) in enumerate(zip(small_hbm, small_refs))
    ]
    for copy in small_loads:
        copy.start()
    layers, channels, columns = jac_ref.shape
    padded = jac_vmem.shape[0]
    bounds = [layers // SUB * (i + 1) // LOADS * SUB for i in range(LOADS - 1)]
    bounds = list(zip([0] + bounds, bounds + [layers]))
    loads = [
        pltpu.make_async_copy(jac_ref.at[pl.ds(a, b - a)], jac_vmem.at[pl.ds(a, b - a)], load_sem.at[i])
        for i, (a, b) in enumerate(bounds)
    ]
    for copy in loads:
        copy.start()
    chunk_count = padded // SUB
    piece_count = len(PIECES)
    half_obs = obs_count // 2
    group = half_obs * chan_count
    rows = kernel_ref.shape[0]
    lows = chan_count // 2
    block_count = columns // BLOCK
    mine = block_count * SUB

    obs, chan = lax.axis_index("obs"), lax.axis_index("chan")
    top = obs // half_obs
    me = (obs % half_obs) * chan_count + chan
    slot = (chan % lows) * (2 * half_obs) + (chan // lows) * half_obs + obs % half_obs

    def coords(member):
        return (top * half_obs + member // chan_count, member % chan_count)

    def other(k):
        member, place = 0, 1
        while place < group:
            member = member + (me // place + k // place) % 2 * place
            place *= 2
        return member

    device_count = obs_count * chan_count
    rank = obs * chan_count + chan

    def any_other(k):
        member, place = 0, 1
        while place < device_count:
            member = member + (rank // place + k // place) % 2 * place
            place *= 2
        return (member // chan_count, member % chan_count)

    partner = ((obs + half_obs) % obs_count, chan)
    barrier = pltpu.get_barrier_semaphore()

    def greet(k):
        pl.semaphore_signal(barrier, inc=1, device_id=coords(other(k)), device_id_type=MESH)

    for k in far_first(group):
        greet(k)
    pl.semaphore_signal(barrier, inc=1, device_id=partner, device_id_type=MESH)

    chunks = [chunk_count - 1] + list(range(chunk_count - 1))
    starts = [sum(PIECES[:p]) for p in range(piece_count)]
    def one_hot(shape, wanted):
        row = lax.broadcasted_iota(jnp.int32, shape, 0)
        column = lax.broadcasted_iota(jnp.int32, shape, 1)
        return jnp.where(column == wanted(row), 1.0, 0.0).astype(jnp.bfloat16)

    order_ref[...] = one_hot(
        (columns, columns), lambda r: r % mine // SUB * BLOCK + r // mine * SUB + r % SUB
    )
    width = SUB * channels
    back_order_ref[...] = one_hot((width, width), lambda r: r % SUB * channels + r // SUB)

    for copy in small_loads:
        copy.wait()
    place = lax.broadcasted_iota(jnp.int32, (channels, columns), 1)
    weight = jnp.where(place < count_ref[0, 0], obs_weight_ref[...], 0.0)
    weight_high = weight.astype(jnp.bfloat16)
    jac_vmem[layers] = weight_high
    jac_vmem[layers + 1] = (weight - weight_high.astype(jnp.float32)).astype(jnp.bfloat16)
    scaled = (weight * depart_ref[...]).astype(jnp.bfloat16).astype(jnp.float32)

    def source_rows(first, count):
        block = jac_vmem[pl.ds(first, count)].astype(jnp.float32)
        source_ref[pl.ds(first, count)] = jnp.sum(block * scaled[None], axis=1)

    def source_step(q, carry):
        source_rows(q * SUB, SUB)
        return carry

    for copy, (a, b) in zip(loads, bounds):
        copy.wait()
        lax.fori_loop(a // SUB, b // SUB, source_step, 0)
    source_rows(layers // SUB * SUB, layers % SUB)
    mixed_ref[...] = jnp.zeros((channels, columns), jnp.float32)
    for k in range(block_count):
        mixed_ref[0:1, k * BLOCK : (k + 1) * BLOCK] = jnp.full((1, BLOCK), block_ref[0, k].astype(jnp.float32))
    mixed_ref[1 : 1 + layers - LANES] = source_ref[LANES:layers]
    jac_vmem[layers + 2] = mixed_ref[...].astype(jnp.bfloat16)
    source_slots = LANES // channels
    for q in range(source_slots):
        jac_vmem[layers + 3 + q] = source_ref[q * channels : (q + 1) * channels].astype(jnp.bfloat16)
    for extra in range(layers + 3 + source_slots, padded):
        jac_vmem[extra] = jnp.zeros((channels, columns), jnp.bfloat16)

    def span(p):
        return pl.ds(starts[p], PIECES[p])

    def chunks_of(p):
        return [(i, chunks[i]) for i in range(starts[p], starts[p] + PIECES[p])]

    def stage(p):
        for i, chunk in chunks_of(p):
            block = jac_vmem[chunk * SUB : (chunk + 1) * SUB].reshape(width, columns)
            turned = one_hot_dot(order_ref[...], block).astype(jnp.bfloat16)
            put_ref[:, i] = turned.reshape(group, mine, width)

    def send(p):
        def one(k, carry):
            member = other(k)
            pltpu.make_async_remote_copy(
                src_ref=put_ref.at[member, span(p)],
                dst_ref=got_ref.at[slot, span(p)],
                send_sem=jac_send.at[p],
                recv_sem=jac_recv.at[p],
                device_id=coords(member),
                device_id_type=MESH,
            ).start()
            return carry

        lax.fori_loop(1, group, one, 0)
        for i, _ in chunks_of(p):
            got_ref[slot, i] = put_ref[me, i]

    stage(0)
    pl.semaphore_wait(barrier, group)
    for p in range(AHEAD):
        if p:
            stage(p)
        send(p)
    for p in range(AHEAD, piece_count):
        stage(p)

    cov = cov_ref[...]
    gram_ref[...] = jnp.zeros(gram_ref.shape, jnp.float32)
    cov_pad_ref[...] = jnp.zeros(cov_pad_ref.shape, jnp.float32)
    gram = exact_dot(cov, cov, TN)
    gram_ref[0:layers, 0:layers] = gram
    gram_high = gram_ref[...].astype(jnp.bfloat16)
    gram_low = (gram_ref[...] - gram_high.astype(jnp.float32)).astype(jnp.bfloat16)
    gram_parts_ref[...] = jnp.concatenate([gram_high, gram_high, gram_low], axis=1)
    cov_pad_ref[0:layers, 0:layers] = cov
    cov_high = cov_pad_ref[...].astype(jnp.bfloat16)
    cov_low = (cov_pad_ref[...] - cov_high.astype(jnp.float32)).astype(jnp.bfloat16)
    cov_parts_ref[...] = jnp.concatenate([cov_high, cov_high, cov_low], axis=1)

    def take(p):
        others = got_ref.at[pl.ds(0, group - 1), span(p)]
        pltpu.make_async_copy(others, others, jac_recv.at[p]).wait()
        for i, chunk in chunks_of(p):
            block = got_ref[:, i].reshape(group * mine, width)
            turned = one_hot_dot(back_order_ref[...], block)
            for low in range(lows):
                part = turned[:, low * LANES : (low + 1) * LANES].reshape(channels, SUB, LANES)
                kernel_ref[low * channels : (low + 1) * channels, chunk * SUB : (chunk + 1) * SUB, :] = part

    half_rows = padded // 2
    lane = lax.broadcasted_iota(jnp.int32, (half_rows, LANES), 1)
    row_spot = lax.broadcasted_iota(jnp.int32, (half_rows, LANES), 0)

    def terms_copies(step):
        return [
            pltpu.make_async_remote_copy(
                src_ref=ref.at[step, 0], dst_ref=ref.at[step, 1],
                send_sem=term_send.at[step, i], recv_sem=term_recv.at[step, i],
                device_id=partner, device_id_type=MESH,
            )
            for i, ref in enumerate((scale_ref, terms_ref))
        ]

    def put_terms(step, terms):
        summed = terms + pltpu.roll(terms, LANES // 2, 1)
        lower = jnp.where(row_spot < layers - half_rows, summed[half_rows:], 0.0)
        packed = jnp.where(lane < LANES // 2, summed[:half_rows], lower)
        largest = jnp.maximum(jnp.max(jnp.abs(packed), axis=0, keepdims=True), 1e-30)
        scale_ref[step, 0] = largest * (1.0 / LEVELS)
        terms_ref[step, 0] = jnp.round(packed * (LEVELS / largest)).astype(jnp.int32).astype(jnp.int16)
        for copy in terms_copies(step):
            copy.start()

    take(0)
    weight_ref[...] = kernel_ref[:, layers, :] + kernel_ref[:, layers + 1, :]
    id_ref[0] = jnp.broadcast_to(kernel_ref[0, layers + 2 : layers + 3, :], (SUB, LANES))
    id_copy = pltpu.make_async_remote_copy(
        src_ref=id_ref.at[0], dst_ref=id_ref.at[1], send_sem=id_send, recv_sem=id_recv,
        device_id=partner, device_id_type=MESH,
    )
    id_copy.start()

    def low_sum(first, count, layer):
        return sum(
            kernel_ref[low * channels + first : low * channels + first + count, layer, :] for low in range(lows)
        )

    for q in range(source_slots):
        spread_ref[q * channels : (q + 1) * channels] = low_sum(0, channels, layers + 3 + q)
    spread_ref[LANES:padded] = jnp.zeros((padded - LANES, LANES), jnp.float32)
    spread_ref[LANES:layers] = low_sum(1, layers - LANES, layers + 2)
    put_terms(0, spread_ref[...])
    for p in range(AHEAD, piece_count):
        send(p)
    early = piece_count - LATE
    for p in range(1, early):
        take(p)

    id_copy.wait()
    grid_row = lax.broadcasted_iota(jnp.int32, (LANES, LANES), 0)
    grid_lane = lax.broadcasted_iota(jnp.int32, (LANES, LANES), 1)

    def pick_of(which):
        wanted = id_ref[which, 0:1, :].astype(jnp.int32) * SUB + grid_lane % SUB
        return jnp.where(grid_row == wanted, 1.0, 0.0).astype(jnp.bfloat16)

    own_pick = pick_of(0)
    both_picks = jnp.concatenate([own_pick, pick_of(1)], axis=1)
    matched = one_hot_dot(own_pick, both_picks, TN).astype(jnp.bfloat16)
    relation = jnp.concatenate([both_picks, matched], axis=0).astype(jnp.float32)
    relation_lane = lax.broadcasted_iota(jnp.int32, relation.shape, 1) % LANES
    for which in range(2):
        kept = relation_lane // (LANES // 2) == which
        relation_ref[which] = jnp.where(kept, relation, 0.0).astype(jnp.bfloat16)

    zero = jnp.zeros((padded, LANES), jnp.float32)

    def collected(step):
        for copy in terms_copies(step):
            copy.wait()
        both = [terms_ref[step, i].astype(jnp.int32).astype(jnp.float32) * scale_ref[step, i] for i in range(2)]
        both = jnp.concatenate(both, axis=1)
        high = both.astype(jnp.bfloat16)
        low = (both - high.astype(jnp.float32)).astype(jnp.bfloat16)
        parts = jnp.concatenate([high.astype(jnp.float32), low.astype(jnp.float32)], axis=0).astype(jnp.bfloat16)
        sums = [one_hot_dot(parts, relation_ref[which]) for which in range(2)]
        return jnp.concatenate([value[:half_rows] + value[half_rows:] for value in sums], axis=0)

    def put_normal(step, spread):
        def normal_step(n, acc):
            kernel = kernel_ref[n]
            predicted = jnp.sum(kernel * spread, axis=0, keepdims=True)
            return acc + kernel * (predicted * weight_ref[pl.ds(n, 1), :])

        put_terms(step, lax.fori_loop(0, rows, normal_step, zero, unroll=8))

    def predict_all(spread):
        def predict_step(n, square):
            predicted = jnp.sum(kernel_ref[n] * spread, axis=0, keepdims=True)
            scaled = predicted * weight_ref[pl.ds(n, 1), :]
            scaled_ref[pl.ds(n, 1), :] = scaled
            return square + predicted * scaled

        return lax.fori_loop(0, rows, predict_step, zero[:1], unroll=8)

    def put_adjoint(step):
        def adjoint_step(n, acc):
            return acc + kernel_ref[n] * scaled_ref[pl.ds(n, 1), :]

        put_terms(step, lax.fori_loop(0, rows, adjoint_step, zero, unroll=8))

    def two_parts(field):
        high = field.astype(jnp.bfloat16)
        return high, (field - high.astype(jnp.float32)).astype(jnp.bfloat16)

    def parts_dot(map_ref, field):
        high, low = two_parts(field)
        parts = jnp.concatenate([high, low, high], axis=0)
        return one_hot_dot(map_ref[...], parts, (((1,), (0,)), ((), ())))

    def gram_dot(field):
        return parts_dot(gram_parts_ref, field)

    def row_of(a, b):
        return jnp.sum(a * b, axis=0, keepdims=True)

    residual_both = collected(0)
    spread_both = gram_dot(residual_both)
    residual, spread = residual_both[:, :LANES], spread_both[:, :LANES]
    spread_ref[...] = spread_both[:, LANES:]

    def predict(p, begin):
        def predict_step(n, carry):
            total = None if begin else predicted_ref[n]
            for _, chunk in chunks_of(p):
                part = pl.ds(chunk * SUB, SUB)
                product = kernel_ref[n, part, :] * spread_ref[part, :]
                total = product if total is None else total + product
            predicted_ref[n] = total
            return carry

        lax.fori_loop(0, rows, predict_step, 0, unroll=8)

    for p in range(early):
        predict(p, p == 0)
    for p in range(early, piece_count):
        take(p)
        predict(p, False)

    def scale_step(n, carry):
        predicted = jnp.sum(predicted_ref[n], axis=0, keepdims=True)
        scaled_ref[pl.ds(n, 1), :] = predicted * weight_ref[pl.ds(n, 1), :]
        return carry

    lax.fori_loop(0, rows, scale_step, 0, unroll=8)
    put_adjoint(1)
    applied_both = residual_both + collected(1)

    def share_row(ref, send_sem, recv_sem, place, targets):
        copies = [
            pltpu.make_async_remote_copy(
                src_ref=ref.at[place], dst_ref=ref.at[place], send_sem=send_sem, recv_sem=recv_sem,
                device_id=target, device_id_type=MESH,
            )
            for target in targets
        ]
        for copy in copies:
            copy.start()

    def wait_rows(ref, send_sem, recv_sem, count):
        others = ref.at[pl.ds(0, count)]
        pltpu.make_async_copy(others, others, recv_sem).wait()
        pltpu.make_async_copy(others, others, send_sem).wait()

    group_targets = [coords(other(k)) for k in far_first(group)]
    control = direction = image = spread_image = image_applied = None
    norm_last = step_last = None
    for step in range(ITERS - 2):
        applied = applied_both[:, :LANES]
        parts_ref[step, me, 0:1] = row_of(residual, spread)
        parts_ref[step, me, 1:2] = row_of(applied, spread)
        share_row(parts_ref.at[step], sum_send.at[step], sum_recv.at[step], me, group_targets)
        next_spread = gram_dot(applied_both)
        put_normal(step + 2, next_spread[:, LANES:])
        wait_rows(parts_ref.at[step], sum_send.at[step], sum_recv.at[step], group - 1)
        total = jnp.sum(parts_ref[step], axis=0)
        total = jnp.sum(total, axis=1, keepdims=True)
        norm_now, curve = total[0:1], total[1:2]
        if step == 0:
            length = norm_now / curve
            direction, image = residual, applied
            control = length * direction
        else:
            ratio = norm_now / norm_last
            length = norm_now / (curve - ratio * norm_now / step_last)
            direction = residual + ratio * direction
            image = applied + ratio * image
            control = control + length * direction
        residual = residual - length * image
        if step == 0:
            spread_image = next_spread[:, :LANES]
            image_applied = applied_both + collected(step + 2)
        else:
            spread_image = next_spread[:, :LANES] + ratio * spread_image
            image_applied = applied_both + collected(step + 2) + ratio * image_applied
        spread = spread - length * spread_image
        applied_both = applied_both - length * image_applied
        norm_last, step_last = norm_now, length

    applied, image_applied = applied_both[:, :LANES], image_applied[:, :LANES]
    next_spread_both = gram_dot(applied_both)
    square = predict_all(next_spread_both[:, LANES:])
    next_spread = next_spread_both[:, :LANES]
    pairs = (
        (residual, spread), (applied, spread), (image, spread), (applied, next_spread),
        (image, next_spread), (image, spread_image), (image_applied, next_spread), (image_applied, spread_image),
    )
    wide = [row_of(a, b) * 0.5 for a, b in pairs] + [square]
    spot = lax.broadcasted_iota(jnp.int32, (1, LANES), 1)
    row = jnp.zeros((1, LANES), jnp.float32)
    for i, value in enumerate(wide):
        row = jnp.where(spot == i, jnp.sum(value, axis=1, keepdims=True), row)
    finals_ref[rank] = row
    share_row(finals_ref, final_send, final_recv, rank, [any_other(k) for k in far_first(device_count)])
    put_adjoint(ITERS)
    straight = one_hot((LANES, LANES), lambda r: r)
    chosen_row = lax.broadcasted_iota(jnp.int32, (obs_count * SUB, GRID_BLK * LANES), 0)
    chosen_lane = lax.broadcasted_iota(jnp.int32, (obs_count * SUB, GRID_BLK * LANES), 1)
    wanted = (chosen_row // SUB * GRID_BLK + chosen_lane // LANES) * SUB + chosen_row % SUB
    chosen = jnp.where(chosen_lane % LANES == wanted, 1.0, 0.0).astype(jnp.bfloat16)
    seen = gram_dot(jnp.concatenate([control, direction], axis=1))
    control_out, direction_out = seen[:, :LANES], seen[:, LANES:]
    felt = parts_dot(cov_parts_ref, jnp.concatenate([residual, applied, image, image_applied], axis=1))
    residual_felt, applied_felt, image_felt, twice_felt = [felt[:, i * LANES : (i + 1) * LANES] for i in range(4)]
    last_felt = applied_felt + parts_dot(cov_parts_ref, collected(ITERS)[:, :LANES])
    wait_rows(finals_ref, final_send, final_recv, device_count - 1)
    total = jnp.sum(finals_ref[...], axis=0)
    sums = [jnp.sum(jnp.where(spot == i, total, 0.0), axis=1, keepdims=True) for i in range(len(wide))]
    norm_now, curve, rest_image, next_next, image_next, image_image, twice_next, twice_image, square = sums
    ratio = norm_now / norm_last
    length = norm_now / (curve - ratio * norm_now / step_last)
    along = curve + ratio * rest_image
    image_square = next_next + ratio * (2.0 * image_next + ratio * image_image)
    norm_next = norm_now - length * (2.0 * along - length * image_square)
    cross = next_next + ratio * image_next
    image_curve = next_next + square + ratio * (2.0 * twice_next + ratio * twice_image)
    curve_next = curve - length * (2.0 * cross - length * image_curve)
    ratio_next = norm_next / norm_now
    length_next = norm_next / (curve_next - ratio_next * norm_next / length)
    direction_out = spread + ratio * direction_out
    spread_image = next_spread + ratio * spread_image
    control_out = control_out + length * direction_out
    control_out = control_out + length_next * (spread - length * spread_image + ratio_next * direction_out)
    image_felt = applied_felt + ratio * image_felt
    residual_felt = residual_felt - length * image_felt
    applied_felt = applied_felt - length * (last_felt + ratio * twice_felt)
    residual_felt = residual_felt - length_next * (applied_felt + ratio_next * image_felt)
    fields = (control_out, residual_felt)
    tall = jnp.concatenate([field[:LANES] for field in fields], axis=0).astype(jnp.bfloat16)
    turned = one_hot_dot(straight, tall).astype(jnp.bfloat16)
    short = jnp.concatenate([field[LANES:] for field in fields], axis=0)
    shifted = []
    for block in range(GRID_BLK):
        parts = [jnp.zeros((4 * SUB * block, LANES), jnp.float32)] * (block > 0)
        parts += [short, jnp.zeros((LANES - 4 * SUB * (block + 1), LANES), jnp.float32)]
        shifted.append(jnp.concatenate(parts, axis=0))
    shifted = jnp.concatenate(shifted, axis=1).astype(jnp.bfloat16)
    for which in range(2):
        value = turned[:, which * LANES : (which + 1) * LANES].reshape(obs_count, GRID_BLK, SUB, LANES)
        for block in range(GRID_BLK):
            back_ref[0, 0:obs_count, block * 2 + which] = value[:, block]
    value = one_hot_dot(chosen, shifted).astype(jnp.bfloat16)
    back_ref[0, 0:obs_count, 2 * GRID_BLK] = value.reshape(obs_count, SUB, LANES)

    for k in far_first(group):
        member = other(k)
        pltpu.make_async_remote_copy(
            src_ref=back_ref.at[0, top * half_obs + member // chan_count],
            dst_ref=back_ref.at[1, me],
            send_sem=back_send,
            recv_sem=back_recv,
            device_id=coords(member),
            device_id_type=MESH,
        ).start()
    back_ref[1, me] = back_ref[0, obs]
    for p in range(piece_count):
        others = put_ref.at[pl.ds(0, group - 1), span(p)]
        pltpu.make_async_copy(others, others, jac_send.at[p]).wait()
    others = back_ref.at[1, pl.ds(0, group - 1)]
    pltpu.make_async_copy(others, others, back_recv).wait()
    pltpu.make_async_copy(others, others, back_send).wait()
    turned = [
        one_hot_dot(straight, back_ref[1, :, i].reshape(group * SUB, LANES)).astype(jnp.bfloat16)
        for i in range(2 * GRID_BLK + 1)
    ]
    for which, out_ref in enumerate((increment_ref, residual_ref)):
        for block in range(GRID_BLK):
            spots = slice(block * BLOCK, (block + 1) * BLOCK)
            out_ref[0:LANES, spots] = turned[block * 2 + which]
            first = (block * 2 + which) * 2 * SUB
            out_ref[LANES:layers, spots] = turned[2 * GRID_BLK][first : first + layers - LANES]


def half_slice_columns(jacobian, departures, obs_weights, column_count, grid_block, sqrt_cov):
    obs_count, chan_count = lax.axis_size("obs"), lax.axis_size("chan")
    group = obs_count // 2 * chan_count
    capacity, channels, layers = jacobian.shape
    mine = capacity // BLOCK * SUB
    padded = LANES + 2 * SUB
    chunk_count = padded // SUB
    piece_count = len(PIECES)
    rows = channels * chan_count // 2
    width = SUB * channels

    out = pltpu.VMEM((layers, GRID_BLK * BLOCK), jnp.bfloat16)
    hbm = pl.BlockSpec(memory_space=pltpu.HBM)
    vmem = pl.BlockSpec(memory_space=pltpu.VMEM)
    dma = pltpu.SemaphoreType.DMA
    bf16, f32 = jnp.bfloat16, jnp.float32
    increment, residual = pl.pallas_call(
        functools.partial(cg_kernel, obs_count, chan_count),
        out_shape=(out, out),
        in_specs=[hbm] * 6,
        out_specs=(vmem, vmem),
        scratch_shapes=[
            pltpu.VMEM(obs_weights.shape, f32),
            pltpu.VMEM(departures.shape, f32),
            pltpu.SMEM((1,) + column_count.shape, jnp.int32),
            pltpu.SMEM((1,) + grid_block.shape, jnp.int32),
            pltpu.VMEM(sqrt_cov.shape, f32),
            pltpu.VMEM((padded, channels, capacity), bf16),
            pltpu.VMEM((padded, capacity), f32),
            pltpu.VMEM((channels, capacity), f32),
            pltpu.VMEM((group, chunk_count, mine, width), bf16),
            pltpu.VMEM((group, chunk_count, mine, width), bf16),
            pltpu.VMEM((rows, padded, LANES), f32),
            pltpu.VMEM((rows, LANES), f32),
            pltpu.VMEM((capacity, capacity), bf16),
            pltpu.VMEM((width, width), bf16),
            pltpu.VMEM((padded, padded), f32),
            pltpu.VMEM((padded, 3 * padded), bf16),
            pltpu.VMEM((padded, padded), f32),
            pltpu.VMEM((padded, 3 * padded), bf16),
            pltpu.VMEM((padded, LANES), f32),
            pltpu.VMEM((rows, SUB, LANES), f32),
            pltpu.VMEM((rows, LANES), f32),
            pltpu.VMEM((2, 2 * LANES, 2 * LANES), bf16),
            pltpu.VMEM((2, SUB, LANES), f32),
            pltpu.VMEM((STEPS, 2, padded // 2, LANES), jnp.int16),
            pltpu.VMEM((STEPS, 2, 1, LANES), f32),
            pltpu.VMEM((ITERS - 2, group, 2, LANES), f32),
            pltpu.VMEM((obs_count * chan_count, 1, LANES), f32),
            pltpu.VMEM((2, group, 2 * GRID_BLK + 1, SUB, LANES), bf16),
            dma((5,)), dma((LOADS,)),
            dma((piece_count,)), dma((piece_count,)),
            dma, dma,
            dma((STEPS, 2)), dma((STEPS, 2)),
            dma((ITERS - 2,)), dma((ITERS - 2,)),
            dma, dma,
            dma, dma,
        ],
        compiler_params=pltpu.CompilerParams(
            collective_id=0, has_side_effects=True, vmem_limit_bytes=VMEM_BYTES
        ),
    )(jacobian.transpose(2, 1, 0), obs_weights, departures, column_count[None], grid_block[None], sqrt_cov)
    return increment.T.astype(f32), residual.T.astype(f32)


def solution(mesh):
    obs_count, chan_count = mesh.shape["obs"], mesh.shape["chan"]
    group = obs_count // 2 * chan_count

    def plan(jacobian, departures, obs_weights, column_count, grid_block, sqrt_cov):
        capacity, channels, layers = jacobian.shape
        mine = capacity // BLOCK * SUB
        fits = (
            obs_count % 2 == 0
            and chan_count % 2 == 0
            and group * SUB == BLOCK
            and obs_count * mine == LANES
            and obs_count * GRID_BLK * SUB == LANES
            and chan_count == 4
            and channels == 32
            and LANES + SUB < layers <= LANES + 2 * SUB - 7
            and sum(PIECES) * SUB == LANES + 2 * SUB
        )
        chosen = half_slice_columns if fits else exchange_per_step
        return chosen(jacobian, departures, obs_weights, column_count, grid_block, sqrt_cov)

    in_specs = (P("obs", "chan", None), P("chan", "obs"), P("chan", "obs"), P("obs"), P("obs"), P())
    out_specs = (P("obs", None), P("obs", None))
    return jax.shard_map(plan, mesh=mesh, in_specs=in_specs, out_specs=out_specs, check_vma=False)
```
